512 devices in a mesh: gz: 32 (over z, x_lo, core), grp: 16 (over y, x_hi).
Axes of the slice: x: 4 (x_hi: 2, x_lo: 2; x = x_hi * 2 + x_lo), y: 8, z: 8, core: 2. Of those that a mesh axis runs over, the one named last changes fastest.
Arguments:
- volumes: bfloat16 [16, 64, 16, 1024], P('grp', 'gz'), may hold values from -6 to 6
- cotangent: bfloat16 [16, 32, 64, 128], P(None, 'gz', None, 'grp'), may hold values from -6 to 6
- fine_kernel: bfloat16 [1728, 64], replicated, may hold values from -0.15625 to 0.15625
- down_kernel: bfloat16 [512, 128], replicated, may hold values from -0.25 to 0.25
- coarse_kernel: bfloat16 [3456, 128], P(None, 'grp'), may hold values from -0.109375 to 0.109375
Outputs:
- coarse_out: bfloat16 [16, 32, 64, 128], P(None, 'gz', None, 'grp')
- volume_grad: bfloat16 [16, 64, 16, 1024], P('grp', 'gz')
- fine_kernel_grad: float32 [1728, 64], replicated
- down_kernel_grad: float32 [512, 128], replicated
- coarse_kernel_grad: float32 [3456, 128], P(None, 'grp')
The draws below stay inside these ranges and needn't reach their ends.
All inputs are finite; a program needn't handle non-finite values.
Results may differ from the reference program's by a relative error of at most 0.019.
Values may be sent and summed in bfloat16 or wider, within the bound.
No kernel may reach another device: no remote copies, remote signals or barrier semaphores. Data moves between devices by JAX's collectives and lax.ppermute only.
A program may use at most 64 MiB of HBM per device.

```python
import jax
import jax.numpy as jnp
from jax import lax

CFINE = 64
CCOARSE = 128
XFINE = 16
YFINE = 16
SAMPLES = 16
ZFINE = 64
ZCOARSE = 32
XYCOARSE = 64


def levels(rng, dims, cuts, smallest, high):
    def one(position, blocks):
        draws = jax.random.uniform(jax.random.fold_in(jax.random.fold_in(rng, 6), position), (blocks,), jnp.float32, smallest / len(cuts), high / len(cuts))
        return jnp.repeat(jnp.exp(draws), dims[position] // blocks).reshape((-1,) + (1,) * (len(dims) - position - 1))

    level = one(*cuts[0])
    for cut in cuts[1:]:
        level = level * one(*cut)
    return level


def bell_draw(own_key, extent, width, most, cuts=(), kind=jnp.bfloat16):
    drawn = jax.random.normal(own_key, extent, jnp.float32) * width
    if len(cuts) > 0:
        drawn = levels(own_key, extent, cuts, -0.22, 0.18) * drawn
    return jnp.clip(drawn, min=-most, max=most).astype(kind)


def setup_inputs(seed: int = 0) -> dict:
    arg_keys = jax.random.split(jax.random.key(seed), 6)
    volumes = bell_draw(arg_keys[0], (SAMPLES, ZFINE, XFINE, YFINE * CFINE), 1.0, 6.0, ((0, 16), (1, 32)))
    cotangent = bell_draw(arg_keys[1], (SAMPLES, ZCOARSE, XYCOARSE, CCOARSE), 1.0, 6.0, ((1, 32), (3, 16)))
    fine_kernel = bell_draw(arg_keys[2], (27 * CFINE, CFINE), (27 * CFINE) ** -0.5, 0.15625)
    down_kernel = bell_draw(arg_keys[3], (8 * CFINE, CCOARSE), (8 * CFINE) ** -0.5, 0.25)
    coarse_kernel = bell_draw(arg_keys[4], (27 * CCOARSE, CCOARSE), (27 * CCOARSE) ** -0.5, 0.109375, ((1, 16),))
    return {"volumes": volumes, "cotangent": cotangent, "fine_kernel": fine_kernel, "down_kernel": down_kernel, "coarse_kernel": coarse_kernel}


def pad_sides(block):
    return jnp.pad(block, ((0, 0), (1, 1), (1, 1), (1, 1), (0, 0)))


def convolve(padded, kernel):
    samples, extent_z, extent_x, extent_y, channels = padded.shape
    extent_z, extent_x, extent_y = extent_z - 2, extent_x - 2, extent_y - 2
    summed = None
    for plane in range(3):
        pieces = [padded[:, plane:plane + extent_z, row_step:row_step + extent_x, col_step:col_step + extent_y, :]
                  for row_step in range(3) for col_step in range(3)]
        columns = jnp.concatenate(pieces, axis=-1).reshape(-1, 9 * channels)
        rows = kernel[plane * 9 * channels:(plane + 1) * 9 * channels]
        partial_value = jnp.dot(columns, rows, preferred_element_type=jnp.float32)
        summed = partial_value if summed is None else summed + partial_value
    return summed.reshape(samples, extent_z, extent_x, extent_y, -1)


def kernel_gradient(padded, grad):
    samples, extent_z, extent_x, extent_y, channels = padded.shape
    extent_z, extent_x, extent_y = extent_z - 2, extent_x - 2, extent_y - 2
    flat_grad = grad.reshape(-1, grad.shape[-1])
    blocks = []
    for plane in range(3):
        pieces = [padded[:, plane:plane + extent_z, row_step:row_step + extent_x, col_step:col_step + extent_y, :]
                  for row_step in range(3) for col_step in range(3)]
        columns = jnp.concatenate(pieces, axis=-1).reshape(-1, 9 * channels)
        blocks.append(lax.dot_general(columns, flat_grad, (((0,), (0,)), ((), ())), preferred_element_type=jnp.float32))
    return jnp.concatenate(blocks, axis=0)


def flip_kernel(kernel, inputs):
    outputs = kernel.shape[1]
    shaped = kernel.reshape(3, 3, 3, inputs, outputs)[::-1, ::-1, ::-1]
    return jnp.transpose(shaped, (0, 1, 2, 4, 3)).reshape(27 * outputs, inputs)


def silu_slope(value):
    sigmoid_v = jax.nn.sigmoid(value)
    return sigmoid_v * (1.0 + value * (1.0 - sigmoid_v))


def pool_columns(block):
    samples, extent_z, extent_x, extent_y, channels = block.shape
    shaped = block.reshape(samples, extent_z // 2, 2, extent_x // 2, 2, extent_y // 2, 2, channels)
    return jnp.transpose(shaped, (0, 1, 3, 5, 2, 4, 6, 7)).reshape(-1, 8 * channels)


def unpool_columns(flat, samples, extent_z, extent_x, extent_y, channels):
    shaped = flat.reshape(samples, extent_z // 2, extent_x // 2, extent_y // 2, 2, 2, 2, channels)
    return jnp.transpose(shaped, (0, 1, 4, 2, 5, 3, 6, 7)).reshape(samples, extent_z, extent_x, extent_y, channels)


def one_volume(volume, grad_out, fine_kernel, down_kernel, coarse_kernel):
    cfine = fine_kernel.shape[1]
    extent_z, extent_x, packed = volume.shape
    extent_y = packed // cfine
    fine = volume.reshape(1, extent_z, extent_x, extent_y, cfine)
    fine_padded = pad_sides(fine)
    fine_pre = convolve(fine_padded, fine_kernel)
    fine_act = jax.nn.silu(fine_pre).astype(jnp.bfloat16)
    pooled = pool_columns(fine_act)
    coarse_in = jnp.dot(pooled, down_kernel, preferred_element_type=jnp.float32).astype(jnp.bfloat16)
    coarse_in = coarse_in.reshape(1, extent_z // 2, extent_x // 2, extent_y // 2, -1)
    coarse_padded = pad_sides(coarse_in)
    coarse_pre = convolve(coarse_padded, coarse_kernel)
    coarse_out = jax.nn.silu(coarse_pre).astype(jnp.bfloat16)
    grad_shaped = grad_out.reshape(coarse_pre.shape).astype(jnp.float32)
    coarse_grad = (grad_shaped * silu_slope(coarse_pre)).astype(jnp.bfloat16)
    coarse_kg = kernel_gradient(coarse_padded, coarse_grad)
    coarse_in_grad = convolve(pad_sides(coarse_grad), flip_kernel(coarse_kernel, coarse_kernel.shape[1])).astype(jnp.bfloat16)
    flat_in_grad = coarse_in_grad.reshape(-1, coarse_in_grad.shape[-1])
    pooled_grad = jnp.dot(flat_in_grad, down_kernel.T, preferred_element_type=jnp.float32)
    fine_act_grad = unpool_columns(pooled_grad, 1, extent_z, extent_x, extent_y, cfine)
    down_kg = lax.dot_general(pooled, flat_in_grad, (((0,), (0,)), ((), ())), preferred_element_type=jnp.float32)
    fine_grad = (fine_act_grad * silu_slope(fine_pre)).astype(jnp.bfloat16)
    fine_kg = kernel_gradient(fine_padded, fine_grad)
    volume_grad = convolve(pad_sides(fine_grad), flip_kernel(fine_kernel, cfine)).astype(jnp.bfloat16)
    out_flat = coarse_out.reshape(extent_z // 2, (extent_x // 2) * (extent_y // 2), -1)
    return out_flat, volume_grad.reshape(extent_z, extent_x, packed), fine_kg, down_kg, coarse_kg


def reference(volumes, cotangent, fine_kernel, down_kernel, coarse_kernel):
    def step(carry, inputs):
        volume, grad_out = inputs
        out_flat, volume_grad, fine_kg, down_kg, coarse_kg = one_volume(volume, grad_out, fine_kernel, down_kernel, coarse_kernel)
        carry = (carry[0] + fine_kg, carry[1] + down_kg, carry[2] + coarse_kg)
        return carry, (out_flat, volume_grad)

    start = (jnp.zeros(fine_kernel.shape, jnp.float32), jnp.zeros(down_kernel.shape, jnp.float32),
             jnp.zeros(coarse_kernel.shape, jnp.float32))
    sums, stacked = lax.scan(step, start, (volumes, cotangent))
    return stacked[0], stacked[1], sums[0], sums[1], sums[2]
```

```python
import jax
import jax.numpy as jnp
from jax import lax
from jax.sharding import PartitionSpec as P


def with_halo(array, sides, width):
    for axis, dim in sides:
        devices, length = (lax.axis_size(axis), array.shape[dim])
        up = [(i, (i + 1) % devices) for i in range(devices - 1)]
        down = [(j, i) for i, j in up]
        last = lax.slice_in_dim(array, length - width, length, axis=dim)
        initial = lax.slice_in_dim(array, 0, width, axis=dim)
        before = lax.ppermute(last, axis, up)
        after = lax.ppermute(initial, axis, down)
        array = jnp.concatenate([before, array, after], axis=dim)
    return array


def in_order(parts, dim):
    dims = list(parts.shape[1:])
    dims[dim] *= parts.shape[0]
    return jnp.moveaxis(parts, 0, dim).reshape(dims)


def from_everyone(array, axis):
    devices = lax.axis_size(axis)
    return lax.all_to_all(
        jnp.broadcast_to(array[None], (devices, *array.shape)), axis, 0, 0, tiled=True
    )


def gathered_copies(array, axis, dim):
    return in_order(from_everyone(array, axis), dim)


def in_blocks(array, dim, devices):
    before, after = (array.shape[:dim], array.shape[dim + 1 :])
    return jnp.moveaxis(array.reshape(*before, devices, -1, *after), dim, 0)


def summed_on_arrival(array, axis, dim):
    devices = lax.axis_size(axis)
    parts = lax.all_to_all(in_blocks(array, dim, devices), axis, 0, 0, tiled=True)
    return jnp.sum(parts.astype(jnp.float32), axis=0)


def pad_sides(block):
    return jnp.pad(block, ((0, 0), (0, 0), (1, 1), (1, 1), (0, 0)))


def convolve(padded, kernel):
    samples, extent_z, extent_x, extent_y, channels = padded.shape
    extent_z, extent_x, extent_y = (extent_z - 2, extent_x - 2, extent_y - 2)
    summed = None
    for plane in range(3):
        pieces = [
            padded[
                :,
                plane : plane + extent_z,
                row_step : row_step + extent_x,
                col_step : col_step + extent_y,
                :,
            ]
            for row_step in range(3)
            for col_step in range(3)
        ]
        columns = jnp.concatenate(pieces, axis=-1).reshape(-1, 9 * channels)
        rows = kernel[plane * 9 * channels : (plane + 1) * 9 * channels]
        partial_value = jnp.dot(columns, rows, preferred_element_type=jnp.float32)
        summed = partial_value if summed is None else summed + partial_value
    return summed.reshape(samples, extent_z, extent_x, extent_y, -1)


def kernel_gradient(padded, grad):
    samples, extent_z, extent_x, extent_y, channels = padded.shape
    extent_z, extent_x, extent_y = (extent_z - 2, extent_x - 2, extent_y - 2)
    flat_grad = grad.reshape(-1, grad.shape[-1])
    blocks = []
    for plane in range(3):
        pieces = [
            padded[
                :,
                plane : plane + extent_z,
                row_step : row_step + extent_x,
                col_step : col_step + extent_y,
                :,
            ]
            for row_step in range(3)
            for col_step in range(3)
        ]
        columns = jnp.concatenate(pieces, axis=-1).reshape(-1, 9 * channels)
        blocks.append(
            lax.dot_general(
                columns, flat_grad, (((0,), (0,)), ((), ())), preferred_element_type=jnp.float32
            )
        )
    return jnp.concatenate(blocks, axis=0)


def flip_kernel(kernel, inputs):
    outputs = kernel.shape[1]
    shaped = kernel.reshape(3, 3, 3, inputs, outputs)[::-1, ::-1, ::-1]
    return jnp.transpose(shaped, (0, 1, 2, 4, 3)).reshape(27 * outputs, inputs)


def silu_slope(value):
    sigmoid_v = jax.nn.sigmoid(value)
    return sigmoid_v * (1.0 + value * (1.0 - sigmoid_v))


def pool_columns(block):
    samples, extent_z, extent_x, extent_y, channels = block.shape
    shaped = block.reshape(samples, extent_z // 2, 2, extent_x // 2, 2, extent_y // 2, 2, channels)
    return jnp.transpose(shaped, (0, 1, 3, 5, 2, 4, 6, 7)).reshape(-1, 8 * channels)


def unpool_columns(flat, samples, extent_z, extent_x, extent_y, channels):
    shaped = flat.reshape(samples, extent_z // 2, extent_x // 2, extent_y // 2, 2, 2, 2, channels)
    return jnp.transpose(shaped, (0, 1, 4, 2, 5, 3, 6, 7)).reshape(
        samples, extent_z, extent_x, extent_y, channels
    )


def coarse_rim(block):
    return with_halo(block, (("gz", 1),), 1)


def coarse_grad_rim(block):
    return with_halo(block, (("gz", 1),), 1)


def gathered(block, axis):
    return from_everyone(block, axis)


def total_over_slice(fine_kg, down_kg, coarse_kg):
    half = fine_kg.shape[0] // 2
    packed_fine = jnp.concatenate([fine_kg[:half], fine_kg[half:]], axis=1)
    shared = jnp.concatenate([packed_fine, down_kg], axis=0)
    local = coarse_kg.T.reshape(-1, 128)
    slabs = lax.axis_size("gz")
    rows = -(-shared.shape[0] // (8 * slabs)) * 8
    own_rows = -(-local.shape[0] // (8 * slabs)) * 8
    shared_blocks = jnp.pad(shared, ((0, rows * slabs - shared.shape[0]), (0, 0)))
    local_blocks = jnp.pad(local, ((0, own_rows * slabs - local.shape[0]), (0, 0)))
    blocks = jnp.concatenate(
        [shared_blocks.reshape(slabs, rows, 128), local_blocks.reshape(slabs, own_rows, 128)], axis=1
    ).astype(jnp.bfloat16)
    arrived = lax.all_to_all(blocks, "gz", 0, 0, tiled=True).astype(jnp.float32).sum(axis=0)
    arrived = arrived.astype(jnp.bfloat16)
    everyone = gathered(arrived[:rows], "grp").astype(jnp.float32).sum(axis=0)
    final = jnp.concatenate([everyone.astype(jnp.bfloat16), arrived[rows:]], axis=0)
    final = gathered(final, "gz").astype(jnp.float32)
    shared_final = final[:, :rows].reshape(-1, 128)
    local_final = final[:, rows:].reshape(-1, 128)[: local.shape[0]]
    fine_total = shared_final[:half]
    fine_total = jnp.concatenate([fine_total[:, :64], fine_total[:, 64:]], axis=0)
    down_total = shared_final[half : half + down_kg.shape[0]]
    coarse_total = local_final.reshape(coarse_kg.shape[1], coarse_kg.shape[0]).T
    return fine_total, down_total, coarse_total


def per_device(volumes, cotangent, fine_kernel, down_kernel, coarse_kernel):
    samples, planes, xfine, packed = volumes.shape
    cfine = fine_kernel.shape[1]
    yfine = packed // cfine
    fine = volumes.reshape(samples, planes, xfine, yfine, cfine)
    fine_padded = pad_sides(with_halo(fine, (("gz", 1),), 1))
    fine_pre = convolve(fine_padded, fine_kernel)
    fine_act = jax.nn.silu(fine_pre).astype(jnp.bfloat16)
    pooled = pool_columns(fine_act)
    coarse_in = jnp.dot(pooled, down_kernel, preferred_element_type=jnp.float32).astype(
        jnp.bfloat16
    )
    coarse_in = coarse_in.reshape(samples, planes // 2, xfine // 2, yfine // 2, -1)
    coarse_framed = coarse_rim(coarse_in)
    full_kernel = gathered_copies(coarse_kernel, "grp", 1)
    own_padded = pad_sides(coarse_framed)
    coarse_pre = convolve(own_padded, full_kernel)
    group, zcoarse, xcoarse, ycoarse, all_channels = coarse_pre.shape
    own_out = (
        jax.nn.silu(coarse_pre)
        .astype(jnp.bfloat16)
        .reshape(group, zcoarse, xcoarse * ycoarse, all_channels)
    )
    coarse_out = lax.all_to_all(own_out, "grp", split_axis=3, concat_axis=0, tiled=True)
    grad_own = lax.all_to_all(cotangent, "grp", split_axis=0, concat_axis=3, tiled=True)
    grad_shaped = grad_own.reshape(coarse_pre.shape).astype(jnp.float32)
    coarse_grad = (grad_shaped * silu_slope(coarse_pre)).astype(jnp.bfloat16)
    whole_kg = kernel_gradient(own_padded, coarse_grad)
    coarse_kg = summed_on_arrival(whole_kg.astype(jnp.bfloat16), "grp", 1)
    partial_value = convolve(
        pad_sides(coarse_grad_rim(coarse_grad)), flip_kernel(full_kernel, all_channels)
    )
    coarse_in_grad = partial_value.astype(jnp.bfloat16)
    flat_in_grad = coarse_in_grad.reshape(-1, coarse_in_grad.shape[-1])
    pooled_grad = jnp.dot(flat_in_grad, down_kernel.T, preferred_element_type=jnp.float32)
    fine_act_grad = unpool_columns(pooled_grad, samples, planes, xfine, yfine, cfine)
    down_kg = lax.dot_general(
        pooled, flat_in_grad, (((0,), (0,)), ((), ())), preferred_element_type=jnp.float32
    )
    fine_grad = (fine_act_grad * silu_slope(fine_pre)).astype(jnp.bfloat16)
    fine_kg = kernel_gradient(fine_padded, fine_grad)
    fine_kg, down_kg, coarse_kg = total_over_slice(fine_kg, down_kg, coarse_kg)
    grad_padded = pad_sides(with_halo(fine_grad, (("gz", 1),), 1))
    volume_grad = convolve(grad_padded, flip_kernel(fine_kernel, cfine)).astype(jnp.bfloat16)
    volume_grad = volume_grad.reshape(samples, planes, xfine, packed)
    return (coarse_out, volume_grad, fine_kg, down_kg, coarse_kg)


def solution(mesh):
    in_specs = (P("grp", "gz", None, None), P(None, "gz", None, "grp"), P(), P(), P(None, "grp"))
    out_specs = (P(None, "gz", None, "grp"), P("grp", "gz", None, None), P(), P(), P(None, "grp"))
    return jax.shard_map(
        per_device, mesh=mesh, in_specs=in_specs, out_specs=out_specs, check_vma=False
    )
```

```python
import jax
import jax.numpy as jnp
from jax import lax
from jax.experimental import pallas as pl
from jax.experimental.pallas import tpu as pltpu
from jax.sharding import PartitionSpec as P

F32 = jnp.float32
BF16 = jnp.bfloat16
NN = (((1,), (0,)), ((), ()))
NT = (((1,), (1,)), ((), ()))
TN = (((0,), (0,)), ((), ()))


def mm(left, right, dims):
    return lax.dot_general(left, right, dims, preferred_element_type=F32)


def shift_rows(value, by, period):
    total = value.shape[0]
    place = lax.broadcasted_iota(jnp.int32, value.shape, 0) % period
    inside = place != (0 if by == 1 else period - 1)
    return jnp.where(inside, pltpu.roll(value, by % total, 0), 0.0)


def low_half(rows):
    return lax.broadcasted_iota(jnp.int32, (rows, 128), 1) < 64


def slope_and_silu(pre):
    sig = jax.nn.sigmoid(pre)
    return sig * (1.0 + pre * (1.0 - sig)), pre * sig


def fill_windows(windows, plane, blocks):
    low = low_half(16)
    none = jnp.zeros((16, 128), BF16)
    for j in range(8):
        after = blocks[j + 1] if j < 7 else none
        before = blocks[j - 1] if j > 0 else none
        rows = pl.ds(j * 16, 16)
        windows[plane, rows, 0:128] = blocks[j]
        windows[plane, rows, 128:256] = jnp.where(low, after, before)


def window_conv(windows, weights, dims):
    parts = []
    for dx in range(3):
        total = None
        for dz in range(3):
            rows = windows[dz : dz + 2].reshape(256, 256)
            term = mm(rows, weights[dz * 3 + dx], dims)
            total = term if total is None else total + term
        parts.append(total)
    return parts[1] + shift_rows(parts[0], 1, 16) + shift_rows(parts[2], -1, 16)


def place_weights(kernel, ahead, behind):
    low = low_half(64)
    tiles = [kernel[:, m * 128 : (m + 1) * 128].astype(F32) for m in range(13)]
    last = kernel[:, 1664:1728].astype(F32)
    tiles.append(jnp.concatenate([last, jnp.zeros((64, 64), F32)], axis=1))
    for k in range(9):
        first, second = tiles[3 * k // 2], tiles[3 * k // 2 + 1]
        swapped = pltpu.roll(jnp.where(low, second, first), 64, 1)
        if k % 2 == 0:
            zero_one, two_none = first, jnp.where(low, second, 0.0)
            one_two, none_zero = swapped, pltpu.roll(jnp.where(low, first, 0.0), 64, 1)
        else:
            one_two, none_zero = second, jnp.where(low, 0.0, first)
            zero_one, two_none = swapped, pltpu.roll(jnp.where(low, 0.0, second), 64, 1)
        blocks = [part.astype(BF16) for part in (one_two, zero_one, none_zero, two_none)]
        ahead[k, 0:64, 0:128] = blocks[0]
        ahead[k, 64:128, 0:128] = blocks[1]
        ahead[k, 0:64, 128:256] = blocks[2]
        ahead[k, 64:128, 128:256] = blocks[3]
        for slot in range(4):
            behind[8 - k, slot * 64 : (slot + 1) * 64] = blocks[slot]


def fine_forward(vol, before, after, weights, down, coarse, slope, windows, pooled, act):
    def lanes(ref, j):
        return ref[:, j * 128 : (j + 1) * 128]

    fill_windows(windows, 0, [lanes(before, j) for j in range(8)])
    fill_windows(windows, 1, [vol[0, :, j * 128 : (j + 1) * 128] for j in range(8)])
    fill_windows(windows, 2, [vol[1, :, j * 128 : (j + 1) * 128] for j in range(8)])
    fill_windows(windows, 3, [lanes(after, j) for j in range(8)])
    pre = window_conv(windows, weights, NT)
    slopes, silu = slope_and_silu(pre)
    slope[...] = slopes
    act[...] = silu
    for z in range(2):
        for bx in range(2):
            part = act[pl.ds(z * 128 + bx, 64, stride=2), :]
            at = (z * 2 + bx) * 128
            pooled[:, at : at + 128] = part.astype(BF16)
    coarse[...] = mm(pooled[...], down[...], NN).astype(BF16)


def y_taps(plane):
    value = plane[...].astype(F32)
    edge = jnp.zeros((8, 128), F32)
    earlier = jnp.concatenate([edge, value[:-8]], axis=0)
    later = jnp.concatenate([value[8:], edge], axis=0)
    return jnp.concatenate([earlier, value, later], axis=1).astype(BF16)


def coarse_forward(own, before, after, packed, grad, out, scratch):
    planes = [y_taps(before), y_taps(own), y_taps(after)]
    parts = []
    for dx in range(3):
        total = None
        for dz in range(3):
            at = (dz * 3 + dx) * 384
            term = mm(planes[dz], packed[:, at : at + 384], NT)
            total = term if total is None else total + term
        parts.append(total)
    pre = parts[1] + shift_rows(parts[0], 1, 8) + shift_rows(parts[2], -1, 8)
    slopes, silu = slope_and_silu(pre)
    scratch[0:64] = silu
    by_x = [scratch[pl.ds(x, 8, stride=8), :] for x in range(8)]
    ordered = jnp.concatenate(by_x + [jnp.zeros((64, 128), F32)], axis=0)
    out[...] = ordered.T.astype(BF16)
    scratch[...] = packed[:, 3456:3584].astype(F32).T
    cotangent = jnp.concatenate([scratch[pl.ds(y, 8, stride=8), :] for y in range(8)], axis=0)
    grad[...] = (cotangent * slopes).astype(BF16)


def coarse_kernel_terms(own, before, after, grad, terms):
    value = grad[...].astype(F32)
    moved = [shift_rows(value, -1, 8), value, shift_rows(value, 1, 8)]
    moved = jnp.concatenate(moved, axis=1).astype(BF16)
    for dz, plane in enumerate((before, own, after)):
        block = mm(moved, y_taps(plane), TN)
        for dx in range(3):
            for dy in range(3):
                part = block[dx * 128 : (dx + 1) * 128, dy * 128 : (dy + 1) * 128]
                terms[(dz * 3 + dx) * 3 + dy] = part.astype(BF16)
    for spare in range(27, 32):
        terms[spare] = jnp.zeros((128, 128), BF16)


def backward(own, before, after, packed, pooled, slope, windows, down, shared, fine_grad, act):
    planes = [after[...], own[...], before[...]]
    edge = jnp.zeros((8, 128), F32)
    parts = []
    for dx in range(3):
        total = None
        for dz in range(3):
            at = (dz * 3 + dx) * 384
            term = mm(planes[dz], packed[:, at : at + 384], NN)
            total = term if total is None else total + term
        earlier = jnp.concatenate([total[8:, 0:128], edge], axis=0)
        later = jnp.concatenate([edge, total[:-8, 256:384]], axis=0)
        parts.append(earlier + total[:, 128:256] + later)
    in_grad = parts[1] + shift_rows(parts[0], -1, 8) + shift_rows(parts[2], 1, 8)
    in_grad = in_grad.astype(BF16)
    act_grad = mm(in_grad, down[...], NT)
    for z in range(2):
        for bx in range(2):
            at = (z * 2 + bx) * 128
            act[pl.ds(z * 128 + bx, 64, stride=2), :] = act_grad[:, at : at + 128]
    grad = (act[...] * slope[...]).astype(BF16)
    fine_grad[0] = grad[0:128]
    fine_grad[1] = grad[128:256]
    value = grad.astype(F32)
    moved = [shift_rows(value, -1, 16), value, shift_rows(value, 1, 16)]
    moved = [part.astype(BF16) for part in moved]
    low = low_half(64)
    held = None
    for dz in range(3):
        rows = windows[dz : dz + 2].reshape(256, 256)
        for dx in range(3):
            block = mm(moved[dx], rows, TN)
            u0, u1 = block[0:64, 0:128], block[0:64, 128:256]
            v0, v1 = block[64:128, 0:128], block[64:128, 128:256]
            for dy, (left, right) in enumerate(((u1, v0), (v0, u0), (u0, v1))):
                tap = (dz * 3 + dx) * 3 + dy
                if tap % 2 == 0:
                    held = pltpu.roll(left, 64, 1) + right
                else:
                    high = left + pltpu.roll(right, 64, 1)
                    at = (tap // 2) * 64
                    shared[at : at + 64] = jnp.where(low, held, high).astype(BF16)
    shared[832:896] = jnp.where(low, held, 0.0).astype(BF16)
    shared[896:1408] = mm(pooled[...], in_grad, TN).astype(BF16)
    shared[1408:1536] = jnp.zeros((128, 128), BF16)


def fine_backward(grad, before, after, weights, out, windows):
    def blocks(plane):
        return [plane[j * 16 : (j + 1) * 16] for j in range(8)]

    fill_windows(windows, 0, blocks(before[...]))
    fill_windows(windows, 1, blocks(grad[0]))
    fill_windows(windows, 2, blocks(grad[1]))
    fill_windows(windows, 3, blocks(after[...]))
    total = window_conv(windows, weights, NN).astype(BF16)
    for z in range(2):
        for j in range(8):
            at = z * 128 + j * 16
            out[z, :, j * 128 : (j + 1) * 128] = total[at : at + 16]


def sum_slabs(terms, shared, features, out):
    def total(ref, at):
        return jnp.sum(ref[:, at : at + 16, :].astype(F32), axis=0)

    for pair in range(8):
        both = total(terms, pair * 16)
        for half in range(2):
            at = pair * 2 + half
            rows = [both[half * 8 : half * 8 + 8], features[at * 8 : at * 8 + 8].astype(F32)]
            out[at, 0:16] = jnp.concatenate(rows, axis=0).astype(BF16)
    for part in range(3):
        rows = total(shared, part * 16).astype(BF16)
        for at in range(16):
            out[at, 16 + part * 16 : 32 + part * 16] = rows


def sum_groups(parts, features, out):
    mixed = parts[:, 0:16, :].astype(F32)
    own = jnp.sum(mixed[:, 0:8], axis=0).astype(BF16)
    for at in range(16):
        features[at] = mixed[at, 8:16, 0:64].astype(BF16)
    rows = [
        jnp.sum(parts[:, 16 + part * 16 : 32 + part * 16, :].astype(F32), axis=0).astype(BF16)
        for part in range(3)
    ]
    for at in range(32):
        for part in range(3):
            out[at, part * 16 : part * 16 + 16] = rows[part]
        out[at, 48:56] = own


def unpack(parts, fine, down, coarse):
    shared = parts[:, 0:48, :].astype(F32).reshape(1536, 128)
    for tile in range(13):
        fine[:, tile * 128 : (tile + 1) * 128] = shared[tile * 64 : (tile + 1) * 64]
    fine[:, 1664:1728] = shared[832:896, 0:64]
    down[...] = shared[896:1408]
    for tap in range(27):
        coarse[:, tap * 128 : (tap + 1) * 128] = parts[tap, 48:56, :].astype(F32)


def call(body, name, outs, *operands, scratch=()):
    return pl.pallas_call(
        body,
        out_shape=[jax.ShapeDtypeStruct(shape, kind) for shape, kind in outs],
        scratch_shapes=[pltpu.VMEM(shape, kind) for shape, kind in scratch],
        name=name,
        cost_estimate=pl.CostEstimate(flops=WORK, transcendentals=0, bytes_accessed=1 << 20),
        interpret=INTERPRET,
    )(*operands)


INTERPRET = False
WORK = 250_000_000


def from_sides(last, first):
    devices = lax.axis_size("gz")
    up = [(i, i + 1) for i in range(devices - 1)]
    down = [(j, i) for i, j in up]
    return lax.ppermute(last, "gz", up), lax.ppermute(first, "gz", down)


def exchange(blocks, axis):
    return lax.all_to_all(blocks, axis, 0, 0, tiled=True)


def per_device(volumes, cotangent, fine_kernel, down_kernel, coarse_kernel):
    group = lax.axis_size("grp")
    slabs = lax.axis_size("gz")
    vol = volumes[0]
    before, after = from_sides(vol[1], vol[0])
    kernel_rows = jnp.broadcast_to(coarse_kernel.T[None], (group, 8, 3456))
    cot_rows = jnp.pad(jnp.swapaxes(cotangent[:, 0], 1, 2), ((0, 0), (0, 0), (0, 64)))
    packed = exchange(jnp.concatenate([kernel_rows, cot_rows], axis=2), "grp").reshape(128, 3584)
    ahead, behind = call(
        place_weights,
        "place_weights",
        [((9, 128, 256), BF16), ((9, 256, 128), BF16)],
        fine_kernel.T,
    )

    coarse_in, slope, windows, pooled = call(
        fine_forward,
        "fine_forward",
        [((64, 128), BF16), ((256, 128), F32), ((4, 128, 256), BF16), ((64, 512), BF16)],
        vol, before, after, ahead, down_kernel,
        scratch=[((256, 128), F32)],
    )
    in_before, in_after = from_sides(coarse_in, coarse_in)
    coarse_grad, features = call(
        coarse_forward,
        "coarse_forward",
        [((64, 128), BF16), ((128, 128), BF16)],
        coarse_in, in_before, in_after, packed,
        scratch=[((128, 128), F32)],
    )
    grad_before, grad_after = from_sides(coarse_grad, coarse_grad)
    (terms,) = call(
        coarse_kernel_terms,
        "coarse_kernel_terms",
        [((slabs, 128, 128), BF16)],
        coarse_in, in_before, in_after, coarse_grad,
    )
    grad_before, grad_after, terms = lax.optimization_barrier((grad_before, grad_after, terms))
    terms = exchange(terms, "gz")
    shared, fine_grad = call(
        backward,
        "backward",
        [((1536, 128), BF16), ((2, 128, 128), BF16)],
        coarse_grad, grad_before, grad_after, packed, pooled, slope, windows, down_kernel,
        scratch=[((256, 128), F32)],
    )
    shared = exchange(shared.reshape(slabs, 48, 128), "gz")
    fine_before, fine_after = from_sides(fine_grad[1], fine_grad[0])
    (volume_grad,) = call(
        fine_backward,
        "fine_backward",
        [((2, 16, 1024), BF16)],
        fine_grad, fine_before, fine_after, behind,
        scratch=[((4, 128, 256), BF16)],
    )
    (parts,) = call(sum_slabs, "sum_slabs", [((group, 64, 128), BF16)], terms, shared, features)
    parts = exchange(parts, "grp")
    out_rows, final = call(
        sum_groups, "sum_groups", [((group, 8, 64), BF16), ((slabs, 56, 128), BF16)], parts
    )
    final = exchange(final, "gz")
    fine_kg, down_kg, coarse_kg = call(
        unpack, "unpack", [((64, 1728), F32), ((512, 128), F32), ((8, 3456), F32)], final
    )
    coarse_out = jnp.swapaxes(out_rows, 1, 2)[:, None]
    return (coarse_out, volume_grad[None], fine_kg.T, down_kg, coarse_kg.T)


def solution(mesh):
    in_specs = (P("grp", "gz", None, None), P(None, "gz", None, "grp"), P(), P(), P(None, "grp"))
    out_specs = (P(None, "gz", None, "grp"), P("grp", "gz", None, None), P(), P(), P(None, "grp"))
    return jax.shard_map(
        per_device, mesh=mesh, in_specs=in_specs, out_specs=out_specs, check_vma=False
    )
```

```python
import jax
import jax.numpy as jnp
from jax import lax
from jax.experimental import pallas as pl
from jax.experimental.pallas import tpu as pltpu
from jax.sharding import PartitionSpec as P

F32 = jnp.float32
BF16 = jnp.bfloat16
NN = (((1,), (0,)), ((), ()))
NT = (((1,), (1,)), ((), ()))
TN = (((0,), (0,)), ((), ()))


def mm(left, right, dims):
    return lax.dot_general(left, right, dims, preferred_element_type=F32)


def shift_rows(value, by, period):
    total = value.shape[0]
    place = lax.broadcasted_iota(jnp.int32, value.shape, 0) % period
    inside = place != (0 if by == 1 else period - 1)
    return jnp.where(inside, pltpu.roll(value, by % total, 0), 0.0)


def low_half(rows):
    return lax.broadcasted_iota(jnp.int32, (rows, 128), 1) < 64


def slope_and_silu(pre):
    sig = jax.nn.sigmoid(pre)
    return sig * (1.0 + pre * (1.0 - sig)), pre * sig


def fill_windows(windows, plane, blocks):
    low = low_half(16)
    none = jnp.zeros((16, 128), BF16)
    for j in range(8):
        after = blocks[j + 1] if j < 7 else none
        before = blocks[j - 1] if j > 0 else none
        rows = pl.ds(j * 16, 16)
        windows[plane, rows, 0:128] = blocks[j]
        windows[plane, rows, 128:256] = jnp.where(low, after, before)


def window_conv(windows, weights, dims):
    parts = []
    for dx in range(3):
        total = None
        for dz in range(3):
            rows = windows[dz : dz + 2].reshape(256, 256)
            term = mm(rows, weights[dz * 3 + dx], dims)
            total = term if total is None else total + term
        parts.append(total)
    return parts[1] + shift_rows(parts[0], 1, 16) + shift_rows(parts[2], -1, 16)


def place_weights(kernel, ahead, behind):
    low = low_half(64)
    tiles = [kernel[:, m * 128 : (m + 1) * 128].astype(F32) for m in range(13)]
    last = kernel[:, 1664:1728].astype(F32)
    tiles.append(jnp.concatenate([last, jnp.zeros((64, 64), F32)], axis=1))
    for k in range(9):
        first, second = tiles[3 * k // 2], tiles[3 * k // 2 + 1]
        swapped = pltpu.roll(jnp.where(low, second, first), 64, 1)
        if k % 2 == 0:
            zero_one, two_none = first, jnp.where(low, second, 0.0)
            one_two, none_zero = swapped, pltpu.roll(jnp.where(low, first, 0.0), 64, 1)
        else:
            one_two, none_zero = second, jnp.where(low, 0.0, first)
            zero_one, two_none = swapped, pltpu.roll(jnp.where(low, 0.0, second), 64, 1)
        blocks = [part.astype(BF16) for part in (one_two, zero_one, none_zero, two_none)]
        ahead[k, 0:64, 0:128] = blocks[0]
        ahead[k, 64:128, 0:128] = blocks[1]
        ahead[k, 0:64, 128:256] = blocks[2]
        ahead[k, 64:128, 128:256] = blocks[3]
        for slot in range(4):
            behind[8 - k, slot * 64 : (slot + 1) * 64] = blocks[slot]


def fine_forward(vol, before, after, weights, down, coarse, slope, windows, pooled, act):
    def lanes(ref, j):
        return ref[:, j * 128 : (j + 1) * 128]

    fill_windows(windows, 0, [lanes(before, j) for j in range(8)])
    fill_windows(windows, 1, [vol[0, :, j * 128 : (j + 1) * 128] for j in range(8)])
    fill_windows(windows, 2, [vol[1, :, j * 128 : (j + 1) * 128] for j in range(8)])
    fill_windows(windows, 3, [lanes(after, j) for j in range(8)])
    pre = window_conv(windows, weights, NT)
    slopes, silu = slope_and_silu(pre)
    slope[...] = slopes
    act[...] = silu
    for z in range(2):
        for bx in range(2):
            part = act[pl.ds(z * 128 + bx, 64, stride=2), :]
            at = (z * 2 + bx) * 128
            pooled[:, at : at + 128] = part.astype(BF16)
    coarse[...] = mm(pooled[...], down[...], NN).astype(BF16)


def y_taps(plane):
    value = plane[...].astype(F32)
    edge = jnp.zeros((8, 128), F32)
    earlier = jnp.concatenate([edge, value[:-8]], axis=0)
    later = jnp.concatenate([value[8:], edge], axis=0)
    return jnp.concatenate([earlier, value, later], axis=1).astype(BF16)


def coarse_forward(own, before, after, packed, grad, out, scratch):
    planes = [y_taps(before), y_taps(own), y_taps(after)]
    parts = []
    for dx in range(3):
        total = None
        for dz in range(3):
            at = (dz * 3 + dx) * 384
            term = mm(planes[dz], packed[:, at : at + 384], NT)
            total = term if total is None else total + term
        parts.append(total)
    pre = parts[1] + shift_rows(parts[0], 1, 8) + shift_rows(parts[2], -1, 8)
    slopes, silu = slope_and_silu(pre)
    scratch[0:64] = silu
    by_x = [scratch[pl.ds(x, 8, stride=8), :] for x in range(8)]
    scratch[...] = packed[:, 3456:3584].astype(F32).T
    cotangent = jnp.concatenate([scratch[pl.ds(y, 8, stride=8), :] for y in range(8)], axis=0)
    slopes = (cotangent * slopes).astype(BF16)
    grad[...] = slopes
    out[...] = jnp.concatenate(by_x + [slopes.astype(F32)], axis=0).T.astype(BF16)


def assemble(own, features, before, after, out):
    sides = jnp.concatenate([before[...].astype(F32), after[...].astype(F32)], axis=0).T
    for at in range(16):
        rows = slice(at * 8, at * 8 + 8)
        out[at, 0:64] = own[...]
        mixed = jnp.concatenate([features[rows].astype(F32), sides[rows]], axis=0)
        out[at, 64:80] = mixed.astype(BF16)


def coarse_kernel_terms(parts, features, terms, grads, taps):
    low = low_half(8)
    place = lax.broadcasted_iota(jnp.int32, (8, 128), 1) % 8
    for volume in range(16):
        taps[volume * 64 : (volume + 1) * 64] = y_taps(parts[volume, 0:64])
        features[volume] = parts[volume, 64:72, 0:64]
    for pair in range(8):
        first = parts[pair * 2, 64:80].astype(F32)
        second = parts[pair * 2 + 1, 64:80].astype(F32)
        own = jnp.where(low, pltpu.roll(first[0:8], 64, 1), second[0:8])
        before = jnp.where(low, first[8:16], pltpu.roll(second[8:16], 64, 1))
        after = jnp.where(low, pltpu.roll(first[8:16], 64, 1), second[8:16])
        for dz, value in enumerate((after, own, before)):
            earlier = jnp.where(place != 7, pltpu.roll(value, 127, 1), 0.0)
            later = jnp.where(place != 0, pltpu.roll(value, 1, 1), 0.0)
            for dx, moved in enumerate((earlier, value, later)):
                at = (dz * 3 + dx) * 8
                grads[at : at + 8, pair * 128 : (pair + 1) * 128] = moved
    total = mm(grads[...].astype(BF16), taps[...], NN)
    for k in range(9):
        for dy in range(3):
            part = total[k * 8 : k * 8 + 8, dy * 128 : (dy + 1) * 128]
            terms[k * 3 + dy] = part.astype(BF16)
    for spare in range(27, 32):
        terms[spare] = jnp.zeros((8, 128), BF16)


def backward(own, before, after, packed, pooled, slope, windows, down, shared, fine_grad, act):
    planes = [after[...], own[...], before[...]]
    edge = jnp.zeros((8, 128), F32)
    parts = []
    for dx in range(3):
        total = None
        for dz in range(3):
            at = (dz * 3 + dx) * 384
            term = mm(planes[dz], packed[:, at : at + 384], NN)
            total = term if total is None else total + term
        earlier = jnp.concatenate([total[8:, 0:128], edge], axis=0)
        later = jnp.concatenate([edge, total[:-8, 256:384]], axis=0)
        parts.append(earlier + total[:, 128:256] + later)
    in_grad = parts[1] + shift_rows(parts[0], -1, 8) + shift_rows(parts[2], 1, 8)
    in_grad = in_grad.astype(BF16)
    act_grad = mm(in_grad, down[...], NT)
    for z in range(2):
        for bx in range(2):
            at = (z * 2 + bx) * 128
            act[pl.ds(z * 128 + bx, 64, stride=2), :] = act_grad[:, at : at + 128]
    grad = (act[...] * slope[...]).astype(BF16)
    fine_grad[0] = grad[0:128]
    fine_grad[1] = grad[128:256]
    value = grad.astype(F32)
    moved = [shift_rows(value, -1, 16), value, shift_rows(value, 1, 16)]
    moved = [part.astype(BF16) for part in moved]
    low = low_half(64)
    held = None
    for dz in range(3):
        rows = windows[dz : dz + 2].reshape(256, 256)
        for dx in range(3):
            block = mm(moved[dx], rows, TN)
            u0, u1 = block[0:64, 0:128], block[0:64, 128:256]
            v0, v1 = block[64:128, 0:128], block[64:128, 128:256]
            for dy, (left, right) in enumerate(((u1, v0), (v0, u0), (u0, v1))):
                tap = (dz * 3 + dx) * 3 + dy
                if tap % 2 == 0:
                    held = pltpu.roll(left, 64, 1) + right
                else:
                    high = left + pltpu.roll(right, 64, 1)
                    at = (tap // 2) * 64
                    shared[at : at + 64] = jnp.where(low, held, high).astype(BF16)
    shared[832:896] = jnp.where(low, held, 0.0).astype(BF16)
    shared[896:1408] = mm(pooled[...], in_grad, TN).astype(BF16)
    shared[1408:1536] = jnp.zeros((128, 128), BF16)


def fine_backward(grad, before, after, weights, out, windows):
    def blocks(plane):
        return [plane[j * 16 : (j + 1) * 16] for j in range(8)]

    fill_windows(windows, 0, blocks(before[...]))
    fill_windows(windows, 1, blocks(grad[0]))
    fill_windows(windows, 2, blocks(grad[1]))
    fill_windows(windows, 3, blocks(after[...]))
    total = window_conv(windows, weights, NN).astype(BF16)
    for z in range(2):
        for j in range(8):
            at = z * 128 + j * 16
            out[z, :, j * 128 : (j + 1) * 128] = total[at : at + 16]


def sum_of(parts, at):
    return jnp.sum(parts[:, at : at + 16, :].astype(F32), axis=0).astype(BF16)


def sum_slabs(shared, out):
    for at in range(0, 48, 16):
        rows = sum_of(shared, at)
        for device in range(16):
            out[device, at : at + 16] = rows


def sum_groups(shared, terms, out):
    own = jnp.sum(terms[...].astype(F32), axis=0).astype(BF16)
    rows = [sum_of(shared, at) for at in range(0, 48, 16)]
    for device in range(32):
        for part in range(3):
            out[device, part * 16 : part * 16 + 16] = rows[part]
        out[device, 48:56] = own


def unpack(parts, fine, down, coarse):
    shared = parts[:, 0:48, :].astype(F32).reshape(1536, 128)
    for tile in range(13):
        fine[:, tile * 128 : (tile + 1) * 128] = shared[tile * 64 : (tile + 1) * 64]
    fine[:, 1664:1728] = shared[832:896, 0:64]
    down[...] = shared[896:1408]
    for tap in range(27):
        coarse[:, tap * 128 : (tap + 1) * 128] = parts[tap, 48:56, :].astype(F32)


def call(body, name, outs, *operands, scratch=(), final=0):
    place = [jax.ShapeDtypeStruct] * final + [pltpu.VMEM] * (len(outs) - final)
    return pl.pallas_call(
        body,
        out_shape=[put(*out) for put, out in zip(place, outs)],
        scratch_shapes=[pltpu.VMEM(shape, kind) for shape, kind in scratch],
        name=name,
        cost_estimate=pl.CostEstimate(flops=WORK, transcendentals=0, bytes_accessed=1 << 20),
        interpret=INTERPRET,
    )(*[pltpu.with_memory_space_constraint(operand, pltpu.VMEM) for operand in operands])


INTERPRET = False
WORK = 250_000_000


def from_sides(last, first):
    devices = lax.axis_size("gz")
    up = [(i, i + 1) for i in range(devices - 1)]
    down = [(j, i) for i, j in up]
    return lax.ppermute(last, "gz", up), lax.ppermute(first, "gz", down)


def exchange(blocks, axis):
    return lax.all_to_all(blocks, axis, 0, 0, tiled=True)


def per_device(volumes, cotangent, fine_kernel, down_kernel, coarse_kernel):
    group = lax.axis_size("grp")
    slabs = lax.axis_size("gz")
    vol = volumes[0]
    before, after = from_sides(vol[1], vol[0])
    kernel_rows = jnp.broadcast_to(coarse_kernel.T[None], (group, 8, 3456))
    cot_rows = jnp.pad(jnp.swapaxes(cotangent[:, 0], 1, 2), ((0, 0), (0, 0), (0, 64)))
    packed = exchange(jnp.concatenate([kernel_rows, cot_rows], axis=2), "grp").reshape(128, 3584)
    ahead, behind = call(
        place_weights,
        "place_weights",
        [((9, 128, 256), BF16), ((9, 256, 128), BF16)],
        fine_kernel.T,
    )

    coarse_in, slope, windows, pooled = call(
        fine_forward,
        "fine_forward",
        [((64, 128), BF16), ((256, 128), F32), ((4, 128, 256), BF16), ((64, 512), BF16)],
        vol, before, after, ahead, down_kernel,
        scratch=[((256, 128), F32)],
    )
    in_before, in_after = from_sides(coarse_in, coarse_in)
    coarse_grad, features = call(
        coarse_forward,
        "coarse_forward",
        [((64, 128), BF16), ((128, 128), BF16)],
        coarse_in, in_before, in_after, packed,
        scratch=[((128, 128), F32)],
    )
    grad_before, grad_after = from_sides(coarse_grad, coarse_grad)
    (parts,) = call(
        assemble,
        "assemble",
        [((group, 80, 128), BF16)],
        coarse_in, features, grad_before, grad_after,
    )
    parts = exchange(parts, "grp")
    shared, fine_grad = call(
        backward,
        "backward",
        [((1536, 128), BF16), ((2, 128, 128), BF16)],
        coarse_grad, grad_before, grad_after, packed, pooled, slope, windows, down_kernel,
        scratch=[((256, 128), F32)],
    )
    shared = exchange(shared.reshape(slabs, 48, 128), "gz")
    out_rows, terms = call(
        coarse_kernel_terms,
        "coarse_kernel_terms",
        [((group, 8, 64), BF16), ((slabs, 8, 128), BF16)],
        parts,
        scratch=[((72, 1024), F32), ((1024, 384), BF16)],
        final=1,
    )
    terms = exchange(terms, "gz")
    fine_before, fine_after = from_sides(fine_grad[1], fine_grad[0])
    (volume_grad,) = call(
        fine_backward,
        "fine_backward",
        [((2, 16, 1024), BF16)],
        fine_grad, fine_before, fine_after, behind,
        scratch=[((4, 128, 256), BF16)],
        final=1,
    )
    (shared,) = call(sum_slabs, "sum_slabs", [((group, 48, 128), BF16)], shared)
    shared = exchange(shared, "grp")
    (final,) = call(sum_groups, "sum_groups", [((slabs, 56, 128), BF16)], shared, terms)
    final = exchange(final, "gz")
    fine_kg, down_kg, coarse_kg = call(
        unpack,
        "unpack",
        [((64, 1728), F32), ((512, 128), F32), ((8, 3456), F32)],
        final,
        final=3,
    )
    coarse_out = jnp.swapaxes(out_rows, 1, 2)[:, None]
    return (coarse_out, volume_grad[None], fine_kg.T, down_kg, coarse_kg.T)


def solution(mesh):
    in_specs = (P("grp", "gz", None, None), P(None, "gz", None, "grp"), P(), P(), P(None, "grp"))
    out_specs = (P(None, "gz", None, "grp"), P("grp", "gz", None, None), P(), P(), P(None, "grp"))
    return jax.shard_map(
        per_device, mesh=mesh, in_specs=in_specs, out_specs=out_specs, check_vma=False
    )
```

```python
import jax
import jax.numpy as jnp
from jax import lax
from jax.experimental import pallas as pl
from jax.experimental.pallas import tpu as pltpu
from jax.sharding import PartitionSpec as P

F32 = jnp.float32
BF16 = jnp.bfloat16
NN = (((1,), (0,)), ((), ()))
NT = (((1,), (1,)), ((), ()))
TN = (((0,), (0,)), ((), ()))


def mm(left, right, dims):
    return lax.dot_general(left, right, dims, preferred_element_type=F32)


def shift_rows(value, by, period):
    total = value.shape[0]
    place = lax.broadcasted_iota(jnp.int32, value.shape, 0) % period
    inside = place != (0 if by == 1 else period - 1)
    return jnp.where(inside, pltpu.roll(value, by % total, 0), 0.0)


def low_half(rows):
    return lax.broadcasted_iota(jnp.int32, (rows, 128), 1) < 64


def slope_and_silu(pre):
    sig = jax.nn.sigmoid(pre)
    return sig * (1.0 + pre * (1.0 - sig)), pre * sig


def fill_windows(windows, plane, blocks):
    low = low_half(16)
    none = jnp.zeros((16, 128), BF16)
    for j in range(8):
        after = blocks[j + 1] if j < 7 else none
        before = blocks[j - 1] if j > 0 else none
        rows = pl.ds(j * 16, 16)
        windows[plane, rows, 0:128] = blocks[j]
        windows[plane, rows, 128:256] = jnp.where(low, after, before)


def window_conv(windows, weights, dims):
    parts = []
    for dx in range(3):
        total = None
        for dz in range(3):
            rows = windows[dz : dz + 2].reshape(256, 256)
            term = mm(rows, weights[dz * 3 + dx], dims)
            total = term if total is None else total + term
        parts.append(total)
    return parts[1] + shift_rows(parts[0], 1, 16) + shift_rows(parts[2], -1, 16)


def place_weights(kernel, ahead, behind):
    low = low_half(64)
    tiles = [kernel[:, m * 128 : (m + 1) * 128].astype(F32) for m in range(13)]
    last = kernel[:, 1664:1728].astype(F32)
    tiles.append(jnp.concatenate([last, jnp.zeros((64, 64), F32)], axis=1))
    for k in range(9):
        first, second = tiles[3 * k // 2], tiles[3 * k // 2 + 1]
        swapped = pltpu.roll(jnp.where(low, second, first), 64, 1)
        if k % 2 == 0:
            zero_one, two_none = first, jnp.where(low, second, 0.0)
            one_two, none_zero = swapped, pltpu.roll(jnp.where(low, first, 0.0), 64, 1)
        else:
            one_two, none_zero = second, jnp.where(low, 0.0, first)
            zero_one, two_none = swapped, pltpu.roll(jnp.where(low, 0.0, second), 64, 1)
        blocks = [part.astype(BF16) for part in (one_two, zero_one, none_zero, two_none)]
        ahead[k, 0:64, 0:128] = blocks[0]
        ahead[k, 64:128, 0:128] = blocks[1]
        ahead[k, 0:64, 128:256] = blocks[2]
        ahead[k, 64:128, 128:256] = blocks[3]
        for slot in range(4):
            behind[8 - k, slot * 64 : (slot + 1) * 64] = blocks[slot]


def fine_forward(vol, before, after, weights, down, coarse, slope, windows, pooled, act):
    def lanes(ref, j):
        return ref[:, j * 128 : (j + 1) * 128]

    fill_windows(windows, 0, [lanes(before, j) for j in range(8)])
    fill_windows(windows, 1, [vol[0, :, j * 128 : (j + 1) * 128] for j in range(8)])
    fill_windows(windows, 2, [vol[1, :, j * 128 : (j + 1) * 128] for j in range(8)])
    fill_windows(windows, 3, [lanes(after, j) for j in range(8)])
    pre = window_conv(windows, weights, NT)
    slopes, silu = slope_and_silu(pre)
    slope[...] = slopes
    act[...] = silu
    for z in range(2):
        for bx in range(2):
            part = act[pl.ds(z * 128 + bx, 64, stride=2), :]
            at = (z * 2 + bx) * 128
            pooled[:, at : at + 128] = part.astype(BF16)
    coarse[...] = mm(pooled[...], down[...], NN).astype(BF16)


def y_taps(plane):
    value = plane[...].astype(F32)
    edge = jnp.zeros((8, 128), F32)
    earlier = jnp.concatenate([edge, value[:-8]], axis=0)
    later = jnp.concatenate([value[8:], edge], axis=0)
    return jnp.concatenate([earlier, value, later], axis=1).astype(BF16)


HALF = 1792


def spread_half(core, kernel, cotangent, out):
    for at in range(16):
        tail = jnp.concatenate([cotangent[at].astype(F32), jnp.zeros((8, 64), F32)], axis=1)
        out[at, :, HALF : HALF + 128] = tail.astype(BF16)

    @pl.when(core[0] == 0)
    def _():
        for at in range(16):
            out[at, :, 0:HALF] = kernel[:, 0:HALF]

    @pl.when(core[0] == 1)
    def _():
        for at in range(16):
            out[at, :, 0:HALF] = kernel[:, 3456 - HALF : 3456]


def coarse_forward(core, own, before, after, mine, other, grad, out, packed, scratch):
    rest = 3456 - HALF

    @pl.when(core[0] == 0)
    def _():
        packed[:, 0:HALF] = mine[:, 0:HALF]
        packed[:, HALF:3456] = other[:, HALF - rest : HALF]

    @pl.when(core[0] == 1)
    def _():
        packed[:, 0:rest] = other[:, 0:rest]
        packed[:, rest:3456] = mine[:, 0:HALF]

    planes = [y_taps(before), y_taps(own), y_taps(after)]
    parts = []
    for dx in range(3):
        total = None
        for dz in range(3):
            at = (dz * 3 + dx) * 384
            term = mm(planes[dz], packed[:, at : at + 384], NT)
            total = term if total is None else total + term
        parts.append(total)
    pre = parts[1] + shift_rows(parts[0], 1, 8) + shift_rows(parts[2], -1, 8)
    slopes, silu = slope_and_silu(pre)
    scratch[0:64] = silu
    by_x = [scratch[pl.ds(x, 8, stride=8), :] for x in range(8)]
    scratch[...] = mine[:, HALF : HALF + 128].astype(F32).T
    cotangent = jnp.concatenate([scratch[pl.ds(y, 8, stride=8), :] for y in range(8)], axis=0)
    slopes = (cotangent * slopes).astype(BF16)
    grad[...] = slopes
    out[...] = jnp.concatenate(by_x + [slopes.astype(F32)], axis=0).T.astype(BF16)


def coarse_kernel_terms(parts, features, terms, grads, taps):
    low = low_half(8)
    place = lax.broadcasted_iota(jnp.int32, (8, 128), 1) % 8
    for volume in range(16):
        taps[volume * 64 : (volume + 1) * 64] = y_taps(parts[volume, 0:64])
        features[volume] = parts[volume, 64:72, 0:64]
    for pair in range(8):
        first = parts[pair * 2, 64:80].astype(F32)
        second = parts[pair * 2 + 1, 64:80].astype(F32)
        own = jnp.where(low, pltpu.roll(first[0:8], 64, 1), second[0:8])
        before = jnp.where(low, first[8:16], pltpu.roll(second[8:16], 64, 1))
        after = jnp.where(low, pltpu.roll(first[8:16], 64, 1), second[8:16])
        for dz, value in enumerate((after, own, before)):
            earlier = jnp.where(place != 7, pltpu.roll(value, 127, 1), 0.0)
            later = jnp.where(place != 0, pltpu.roll(value, 1, 1), 0.0)
            for dx, moved in enumerate((earlier, value, later)):
                at = (dz * 3 + dx) * 8
                grads[at : at + 8, pair * 128 : (pair + 1) * 128] = moved
    total = mm(grads[...].astype(BF16), taps[...], NN)
    shared = []
    for at in range(80, 176, 16):
        both = jnp.sum(parts[:, at : at + 16, :].astype(F32), axis=0)
        shared += [both[0:8], both[8:16]]
    none = jnp.zeros((8, 128), F32)
    for device in range(32):
        k, dy = divmod(device, 3)
        own = total[k * 8 : k * 8 + 8, dy * 128 : (dy + 1) * 128] if device < 27 else none
        other = shared[device] if device < 12 else none
        terms[device] = jnp.concatenate([own, other], axis=0).astype(BF16)


def backward(
    own, before, after, packed, pooled, slope, windows, down, coarse_in, features,
    out, fine_grad, act, shared,
):
    planes = [after[...], own[...], before[...]]
    edge = jnp.zeros((8, 128), F32)
    parts = []
    for dx in range(3):
        total = None
        for dz in range(3):
            at = (dz * 3 + dx) * 384
            term = mm(planes[dz], packed[:, at : at + 384], NN)
            total = term if total is None else total + term
        earlier = jnp.concatenate([total[8:, 0:128], edge], axis=0)
        later = jnp.concatenate([edge, total[:-8, 256:384]], axis=0)
        parts.append(earlier + total[:, 128:256] + later)
    in_grad = parts[1] + shift_rows(parts[0], -1, 8) + shift_rows(parts[2], 1, 8)
    in_grad = in_grad.astype(BF16)
    act_grad = mm(in_grad, down[...], NT)
    for z in range(2):
        for bx in range(2):
            at = (z * 2 + bx) * 128
            act[pl.ds(z * 128 + bx, 64, stride=2), :] = act_grad[:, at : at + 128]
    grad = (act[...] * slope[...]).astype(BF16)
    fine_grad[0] = grad[0:128]
    fine_grad[1] = grad[128:256]
    value = grad.astype(F32)
    moved = [shift_rows(value, -1, 16), value, shift_rows(value, 1, 16)]
    moved = [part.astype(BF16) for part in moved]
    low = low_half(64)
    held = None
    for dz in range(3):
        rows = windows[dz : dz + 2].reshape(256, 256)
        for dx in range(3):
            block = mm(moved[dx], rows, TN)
            u0, u1 = block[0:64, 0:128], block[0:64, 128:256]
            v0, v1 = block[64:128, 0:128], block[64:128, 128:256]
            for dy, (left, right) in enumerate(((u1, v0), (v0, u0), (u0, v1))):
                tap = (dz * 3 + dx) * 3 + dy
                if tap % 2 == 0:
                    held = pltpu.roll(left, 64, 1) + right
                else:
                    high = left + pltpu.roll(right, 64, 1)
                    at = (tap // 2) * 64
                    shared[at : at + 64] = jnp.where(low, held, high).astype(BF16)
    shared[832:896] = jnp.where(low, held, 0.0).astype(BF16)
    shared[896:1408] = mm(pooled[...], in_grad, TN).astype(BF16)
    shared[1408:1536] = jnp.zeros((128, 128), BF16)
    sides = jnp.concatenate([before[...].astype(F32), after[...].astype(F32)], axis=0).T
    for at in range(16):
        rows = slice(at * 8, at * 8 + 8)
        out[at, 0:64] = coarse_in[...]
        mixed = jnp.concatenate([features[rows].astype(F32), sides[rows]], axis=0)
        out[at, 64:80] = mixed.astype(BF16)
        out[at, 80:176] = shared[at * 96 : at * 96 + 96]


def fine_backward(grad, before, after, weights, out, windows):
    def blocks(plane):
        return [plane[j * 16 : (j + 1) * 16] for j in range(8)]

    fill_windows(windows, 0, blocks(before[...]))
    fill_windows(windows, 1, blocks(grad[0]))
    fill_windows(windows, 2, blocks(grad[1]))
    fill_windows(windows, 3, blocks(after[...]))
    total = window_conv(windows, weights, NN).astype(BF16)
    for z in range(2):
        for j in range(8):
            at = z * 128 + j * 16
            out[z, :, j * 128 : (j + 1) * 128] = total[at : at + 16]


def sum_slabs(terms, out):
    total = jnp.sum(terms[...].astype(F32), axis=0).astype(BF16)
    for device in range(32):
        out[device] = total


def collect(terms, coarse, out):
    rows = []
    for device in range(27):
        both = terms[device].astype(F32)
        coarse[:, device * 128 : (device + 1) * 128] = both[0:8]
        rows.append(both[8:16])
    for pair in range(6):
        both = jnp.concatenate(rows[pair * 2 : pair * 2 + 2], axis=0).astype(BF16)
        for device in range(16):
            out[device, pair * 16 : pair * 16 + 16] = both


def unpack(shared, fine, down):
    for tile in range(13):
        rows = shared[tile * 64 : (tile + 1) * 64]
        fine[:, tile * 128 : (tile + 1) * 128] = rows.astype(F32)
    fine[:, 1664:1728] = shared[832:896].astype(F32)[:, 0:64]
    down[...] = shared[896:1408].astype(F32)


def call(body, name, outs, *operands, scratch=(), far=(), core=None, moved=True):
    place = [jax.ShapeDtypeStruct if at in far else pltpu.VMEM for at in range(len(outs))]
    first = [] if core is None else [core]
    if moved:
        operands = [pltpu.with_memory_space_constraint(part, pltpu.VMEM) for part in operands]
    specs = [pl.BlockSpec(memory_space=pltpu.SMEM) for _ in first]
    return pl.pallas_call(
        body,
        out_shape=[put(*out) for put, out in zip(place, outs)],
        in_specs=specs + [pl.BlockSpec(memory_space=pltpu.VMEM) for _ in operands],
        scratch_shapes=[pltpu.VMEM(shape, kind) for shape, kind in scratch],
        name=name,
        cost_estimate=pl.CostEstimate(flops=WORK, transcendentals=0, bytes_accessed=1 << 20),
        interpret=INTERPRET,
    )(*first, *operands)


INTERPRET = False
WORK = 250_000_000


def from_sides(last, first):
    devices = lax.axis_size("gz")
    up = [(i, i + 1) for i in range(devices - 1)]
    down = [(j, i) for i, j in up]
    return lax.ppermute(last, "gz", up), lax.ppermute(first, "gz", down)


def exchange(blocks, axis):
    return lax.all_to_all(blocks, axis, 0, 0, tiled=True)


def per_device(volumes, cotangent, fine_kernel, down_kernel, coarse_kernel):
    group = lax.axis_size("grp")
    slabs = lax.axis_size("gz")
    vol = volumes[0]
    before, after = from_sides(vol[1], vol[0])
    core = (lax.axis_index("gz") & 1).astype(jnp.int32).reshape(1)
    (halves,) = call(
        spread_half,
        "spread_half",
        [((group, 8, HALF + 128), BF16)],
        coarse_kernel.T, jnp.swapaxes(cotangent[:, 0], 1, 2),
        core=core,
        moved=False,
    )
    mine = exchange(halves, "grp").reshape(128, HALF + 128)
    ahead, behind = call(
        place_weights,
        "place_weights",
        [((9, 128, 256), BF16), ((9, 256, 128), BF16)],
        fine_kernel.T,
        far=(1,),
    )

    coarse_in, slope, windows, pooled = call(
        fine_forward,
        "fine_forward",
        [((64, 128), BF16), ((256, 128), F32), ((4, 128, 256), BF16), ((64, 512), BF16)],
        vol, before, after, ahead, down_kernel,
        scratch=[((256, 128), F32)],
        far=(2,),
    )
    in_before, in_after = from_sides(coarse_in, coarse_in)
    mine, in_before, in_after = lax.optimization_barrier((mine, in_before, in_after))
    other = lax.ppermute(mine, "gz", [(i, i ^ 1) for i in range(slabs)])
    coarse_grad, features, packed = call(
        coarse_forward,
        "coarse_forward",
        [((64, 128), BF16), ((128, 128), BF16), ((128, 3456), BF16)],
        coarse_in, in_before, in_after, mine, other,
        scratch=[((128, 128), F32)],
        core=core,
    )
    grad_before, grad_after = from_sides(coarse_grad, coarse_grad)
    parts, fine_grad = call(
        backward,
        "backward",
        [((group, 176, 128), BF16), ((2, 128, 128), BF16)],
        coarse_grad, grad_before, grad_after, packed, pooled, slope, windows, down_kernel,
        coarse_in, features,
        scratch=[((256, 128), F32), ((1536, 128), BF16)],
    )
    parts = exchange(parts, "grp")
    out_rows, terms = call(
        coarse_kernel_terms,
        "coarse_kernel_terms",
        [((group, 8, 64), BF16), ((slabs, 16, 128), BF16)],
        parts,
        scratch=[((72, 1024), F32), ((1024, 384), BF16)],
        far=(0,),
    )
    terms = exchange(terms, "gz")
    (terms,) = call(sum_slabs, "sum_slabs", [((slabs, 16, 128), BF16)], terms)
    terms = exchange(terms, "gz")
    coarse_kg, shared = call(
        collect, "collect", [((8, 3456), F32), ((group, 96, 128), BF16)], terms, far=(0,)
    )
    shared = exchange(shared, "grp").reshape(1536, 128)
    fine_kg, down_kg = call(
        unpack, "unpack", [((64, 1728), F32), ((512, 128), F32)], shared, far=(0, 1)
    )
    fine_before, fine_after = from_sides(fine_grad[1], fine_grad[0])
    (volume_grad,) = call(
        fine_backward,
        "fine_backward",
        [((2, 16, 1024), BF16)],
        fine_grad, fine_before, fine_after, behind,
        scratch=[((4, 128, 256), BF16)],
        far=(0,),
    )
    coarse_out = jnp.swapaxes(out_rows, 1, 2)[:, None]
    return (coarse_out, volume_grad[None], fine_kg.T, down_kg, coarse_kg.T)


def solution(mesh):
    in_specs = (P("grp", "gz", None, None), P(None, "gz", None, "grp"), P(), P(), P(None, "grp"))
    out_specs = (P(None, "gz", None, "grp"), P("grp", "gz", None, None), P(), P(), P(None, "grp"))
    return jax.shard_map(
        per_device, mesh=mesh, in_specs=in_specs, out_specs=out_specs, check_vma=False
    )
```

```python
import jax
import jax.numpy as jnp
from jax import lax
from jax.experimental import pallas as pl
from jax.experimental.pallas import tpu as pltpu
from jax.sharding import PartitionSpec as P


F32 = jnp.float32
BF16 = jnp.bfloat16
NN = (((1,), (0,)), ((), ()))
NT = (((1,), (1,)), ((), ()))
TN = (((0,), (0,)), ((), ()))


def mm(left, right, dims):
    return lax.dot_general(left, right, dims, preferred_element_type=F32)


def shift_rows(value, by, period):
    total = value.shape[0]
    place = lax.broadcasted_iota(jnp.int32, value.shape, 0) % period
    inside = place != (0 if by == 1 else period - 1)
    return jnp.where(inside, pltpu.roll(value, by % total, 0), 0.0)


def low_half(rows):
    return lax.broadcasted_iota(jnp.int32, (rows, 128), 1) < 64


def slope_and_silu(pre):
    sig = jax.nn.sigmoid(pre)
    return sig * (1.0 + pre * (1.0 - sig)), pre * sig


def fill_windows(windows, plane, blocks):
    low = low_half(16)
    none = jnp.zeros((16, 128), BF16)
    for j in range(8):
        after = blocks[j + 1] if j < 7 else none
        before = blocks[j - 1] if j > 0 else none
        rows = pl.ds(j * 16, 16)
        windows[plane, rows, 0:128] = blocks[j]
        windows[plane, rows, 128:256] = jnp.where(low, after, before)


def window_conv(windows, weights, dims):
    parts = []
    for dx in range(3):
        total = None
        for dz in range(3):
            rows = windows[dz : dz + 2].reshape(256, 256)
            term = mm(rows, weights[dz * 3 + dx], dims)
            total = term if total is None else total + term
        parts.append(total)
    return parts[1] + shift_rows(parts[0], 1, 16) + shift_rows(parts[2], -1, 16)


def place_weights(kernel, ahead, behind):
    low = low_half(64)
    tiles = [kernel[:, m * 128 : (m + 1) * 128].astype(F32) for m in range(13)]
    last = kernel[:, 1664:1728].astype(F32)
    tiles.append(jnp.concatenate([last, jnp.zeros((64, 64), F32)], axis=1))
    for k in range(9):
        first, second = tiles[3 * k // 2], tiles[3 * k // 2 + 1]
        swapped = pltpu.roll(jnp.where(low, second, first), 64, 1)
        if k % 2 == 0:
            zero_one, two_none = first, jnp.where(low, second, 0.0)
            one_two, none_zero = swapped, pltpu.roll(jnp.where(low, first, 0.0), 64, 1)
        else:
            one_two, none_zero = second, jnp.where(low, 0.0, first)
            zero_one, two_none = swapped, pltpu.roll(jnp.where(low, 0.0, second), 64, 1)
        blocks = [part.astype(BF16) for part in (one_two, zero_one, none_zero, two_none)]
        ahead[k, 0:64, 0:128] = blocks[0]
        ahead[k, 64:128, 0:128] = blocks[1]
        ahead[k, 0:64, 128:256] = blocks[2]
        ahead[k, 64:128, 128:256] = blocks[3]
        for slot in range(4):
            behind[8 - k, slot * 64 : (slot + 1) * 64] = blocks[slot]


def fine_forward(vol, before, after, weights, down, coarse, slope, windows, pooled, act):
    def lanes(ref, j):
        return ref[:, j * 128 : (j + 1) * 128]

    fill_windows(windows, 0, [lanes(before, j) for j in range(8)])
    fill_windows(windows, 1, [vol[0, :, j * 128 : (j + 1) * 128] for j in range(8)])
    fill_windows(windows, 2, [vol[1, :, j * 128 : (j + 1) * 128] for j in range(8)])
    fill_windows(windows, 3, [lanes(after, j) for j in range(8)])
    pre = window_conv(windows, weights, NT)
    slopes, silu = slope_and_silu(pre)
    slope[...] = slopes
    act[...] = silu
    for z in range(2):
        for bx in range(2):
            part = act[pl.ds(z * 128 + bx, 64, stride=2), :]
            at = (z * 2 + bx) * 128
            pooled[:, at : at + 128] = part.astype(BF16)
    coarse[...] = mm(pooled[...], down[...], NN).astype(BF16)


def y_taps(plane):
    value = plane[...].astype(F32)
    edge = jnp.zeros((8, 128), F32)
    earlier = jnp.concatenate([edge, value[:-8]], axis=0)
    later = jnp.concatenate([value[8:], edge], axis=0)
    return jnp.concatenate([earlier, value, later], axis=1).astype(BF16)


HALF = 1792


def spread_half(core, kernel, cotangent, out):
    for at in range(16):
        tail = jnp.concatenate([cotangent[at].astype(F32), jnp.zeros((8, 64), F32)], axis=1)
        out[at, :, HALF : HALF + 128] = tail.astype(BF16)

    @pl.when(core[0] == 0)
    def _():
        for at in range(16):
            out[at, :, 0:HALF] = kernel[:, 0:HALF]

    @pl.when(core[0] == 1)
    def _():
        for at in range(16):
            out[at, :, 0:HALF] = kernel[:, 3456 - HALF : 3456]


def coarse_forward(core, own, before, after, mine, other, grad, out, packed, scratch):
    rest = 3456 - HALF

    @pl.when(core[0] == 0)
    def _():
        packed[:, 0:HALF] = mine[:, 0:HALF]
        packed[:, HALF:3456] = other[:, HALF - rest : HALF]

    @pl.when(core[0] == 1)
    def _():
        packed[:, 0:rest] = other[:, 0:rest]
        packed[:, rest:3456] = mine[:, 0:HALF]

    planes = [y_taps(before), y_taps(own), y_taps(after)]
    parts = []
    for dx in range(3):
        total = None
        for dz in range(3):
            at = (dz * 3 + dx) * 384
            term = mm(planes[dz], packed[:, at : at + 384], NT)
            total = term if total is None else total + term
        parts.append(total)
    pre = parts[1] + shift_rows(parts[0], 1, 8) + shift_rows(parts[2], -1, 8)
    slopes, silu = slope_and_silu(pre)
    scratch[0:64] = silu
    by_x = [scratch[pl.ds(x, 8, stride=8), :] for x in range(8)]
    scratch[...] = mine[:, HALF : HALF + 128].astype(F32).T
    cotangent = jnp.concatenate([scratch[pl.ds(y, 8, stride=8), :] for y in range(8)], axis=0)
    slopes = (cotangent * slopes).astype(BF16)
    grad[...] = slopes
    out[...] = jnp.concatenate(by_x + [slopes.astype(F32)], axis=0).T.astype(BF16)


def coarse_kernel_terms(parts, features, terms, grads, taps):
    low = low_half(8)
    place = lax.broadcasted_iota(jnp.int32, (8, 128), 1) % 8
    for volume in range(16):
        taps[volume * 64 : (volume + 1) * 64] = y_taps(parts[volume, 0:64])
        features[volume] = parts[volume, 64:72, 0:64]
    for pair in range(8):
        first = parts[pair * 2, 64:80].astype(F32)
        second = parts[pair * 2 + 1, 64:80].astype(F32)
        own = jnp.where(low, pltpu.roll(first[0:8], 64, 1), second[0:8])
        before = jnp.where(low, first[8:16], pltpu.roll(second[8:16], 64, 1))
        after = jnp.where(low, pltpu.roll(first[8:16], 64, 1), second[8:16])
        for dz, value in enumerate((after, own, before)):
            earlier = jnp.where(place != 7, pltpu.roll(value, 127, 1), 0.0)
            later = jnp.where(place != 0, pltpu.roll(value, 1, 1), 0.0)
            for dx, moved in enumerate((earlier, value, later)):
                at = (dz * 3 + dx) * 8
                grads[at : at + 8, pair * 128 : (pair + 1) * 128] = moved
    total = mm(grads[...].astype(BF16), taps[...], NN)
    shared = []
    for at in range(80, 160, 16):
        both = jnp.sum(parts[:, at : at + 16, :].astype(F32), axis=0)
        shared += [both[0:8], both[8:16]]
    shared.append(jnp.sum(parts[:, 160:168, :].astype(F32), axis=0))
    none = jnp.zeros((8, 128), F32)
    for device in range(32):
        k, dy = divmod(device, 3)
        own = total[k * 8 : k * 8 + 8, dy * 128 : (dy + 1) * 128] if device < 27 else none
        other = shared[device] if device < 11 else none
        terms[device] = jnp.concatenate([own, other], axis=0).astype(BF16)


def backward(
    own, before, after, packed, pooled, slope, windows, down, coarse_in, features,
    out, fine_grad, act, shared,
):
    planes = [after[...], own[...], before[...]]
    edge = jnp.zeros((8, 128), F32)
    parts = []
    for dx in range(3):
        total = None
        for dz in range(3):
            at = (dz * 3 + dx) * 384
            term = mm(planes[dz], packed[:, at : at + 384], NN)
            total = term if total is None else total + term
        earlier = jnp.concatenate([total[8:, 0:128], edge], axis=0)
        later = jnp.concatenate([edge, total[:-8, 256:384]], axis=0)
        parts.append(earlier + total[:, 128:256] + later)
    in_grad = parts[1] + shift_rows(parts[0], -1, 8) + shift_rows(parts[2], 1, 8)
    in_grad = in_grad.astype(BF16)
    act_grad = mm(in_grad, down[...], NT)
    for z in range(2):
        for bx in range(2):
            at = (z * 2 + bx) * 128
            act[pl.ds(z * 128 + bx, 64, stride=2), :] = act_grad[:, at : at + 128]
    grad = (act[...] * slope[...]).astype(BF16)
    fine_grad[0] = grad[0:128]
    fine_grad[1] = grad[128:256]
    value = grad.astype(F32)
    moved = [shift_rows(value, -1, 16), value, shift_rows(value, 1, 16)]
    moved = [part.astype(BF16) for part in moved]
    low = low_half(64)
    held = None
    for dz in range(3):
        rows = windows[dz : dz + 2].reshape(256, 256)
        for dx in range(3):
            block = mm(moved[dx], rows, TN)
            u0, u1 = block[0:64, 0:128], block[0:64, 128:256]
            v0, v1 = block[64:128, 0:128], block[64:128, 128:256]
            for dy, (left, right) in enumerate(((u1, v0), (v0, u0), (u0, v1))):
                tap = (dz * 3 + dx) * 3 + dy
                if tap % 2 == 0:
                    held = pltpu.roll(left, 64, 1) + right
                else:
                    high = left + pltpu.roll(right, 64, 1)
                    at = (tap // 2) * 64
                    shared[at : at + 64] = jnp.where(low, held, high)
    shared[832:896] = jnp.where(low, held, 0.0)
    shared[896:1408] = mm(pooled[...], in_grad, TN)
    sides = jnp.concatenate([before[...].astype(F32), after[...].astype(F32)], axis=0).T
    for at in range(16):
        rows = slice(at * 8, at * 8 + 8)
        out[at, 0:64] = coarse_in[...]
        mixed = jnp.concatenate([features[rows].astype(F32), sides[rows]], axis=0)
        out[at, 64:80] = mixed.astype(BF16)
        out[at, 80:168] = shared[at * 88 : at * 88 + 88].astype(BF16)


def fine_backward(grad, before, after, weights, out, windows):
    def blocks(plane):
        return [plane[j * 16 : (j + 1) * 16] for j in range(8)]

    fill_windows(windows, 0, blocks(before[...]))
    fill_windows(windows, 1, blocks(grad[0]))
    fill_windows(windows, 2, blocks(grad[1]))
    fill_windows(windows, 3, blocks(after[...]))
    total = window_conv(windows, weights, NN).astype(BF16)
    for z in range(2):
        for j in range(8):
            at = z * 128 + j * 16
            out[z, :, j * 128 : (j + 1) * 128] = total[at : at + 16]


def sum_slabs(terms, out):
    total = jnp.sum(terms[...].astype(F32), axis=0).astype(BF16)
    for device in range(32):
        out[device] = total


def collect(terms, coarse, out):
    rows = []
    for device in range(27):
        both = terms[device].astype(F32)
        coarse[:, device * 128 : (device + 1) * 128] = both[0:8]
        rows.append(both[8:16])
    total = jnp.concatenate(rows[0:11], axis=0).astype(BF16)
    for device in range(16):
        out[device] = total


def unpack(shared, fine, down):
    for tile in range(13):
        rows = shared[tile * 64 : (tile + 1) * 64]
        fine[:, tile * 128 : (tile + 1) * 128] = rows.astype(F32)
    fine[:, 1664:1728] = shared[832:896].astype(F32)[:, 0:64]
    down[...] = shared[896:1408].astype(F32)


def call(body, outs, *operands, scratch=(), far=(), core=None, moved=True):
    place = [jax.ShapeDtypeStruct if at in far else pltpu.VMEM for at in range(len(outs))]
    first = [] if core is None else [core]
    if moved:
        operands = [pltpu.with_memory_space_constraint(part, pltpu.VMEM) for part in operands]
    specs = [pl.BlockSpec(memory_space=pltpu.SMEM) for _ in first]
    return pl.pallas_call(
        body,
        out_shape=[put(*out) for put, out in zip(place, outs)],
        in_specs=specs + [pl.BlockSpec(memory_space=pltpu.VMEM) for _ in operands],
        scratch_shapes=[pltpu.VMEM(shape, kind) for shape, kind in scratch],
        cost_estimate=pl.CostEstimate(flops=WORK, transcendentals=0, bytes_accessed=1 << 20),
        interpret=INTERPRET,
    )(*first, *operands)


INTERPRET = False
WORK = 250_000_000


def from_sides(last, first):
    devices = lax.axis_size("gz")
    up = [(i, i + 1) for i in range(devices - 1)]
    down = [(j, i) for i, j in up]
    return lax.ppermute(last, "gz", up), lax.ppermute(first, "gz", down)


def exchange(blocks, axis):
    return lax.all_to_all(blocks, axis, 0, 0, tiled=True)


def per_device(volumes, cotangent, fine_kernel, down_kernel, coarse_kernel):
    group = lax.axis_size("grp")
    slabs = lax.axis_size("gz")
    vol = volumes[0]
    before, after = from_sides(vol[1], vol[0])
    core = (lax.axis_index("gz") & 1).astype(jnp.int32).reshape(1)
    (halves,) = call(
        spread_half,
        [((group, 8, HALF + 128), BF16)],
        coarse_kernel.T, jnp.swapaxes(cotangent[:, 0], 1, 2),
        core=core,
        moved=False,
    )
    mine = exchange(halves, "grp").reshape(128, HALF + 128)
    ahead, behind = call(
        place_weights, [((9, 128, 256), BF16), ((9, 256, 128), BF16)], fine_kernel.T, far=(1,)
    )

    coarse_in, slope, windows, pooled = call(
        fine_forward,
        [((64, 128), BF16), ((256, 128), F32), ((4, 128, 256), BF16), ((64, 512), BF16)],
        vol, before, after, ahead, down_kernel,
        scratch=[((256, 128), F32)],
        far=(2,),
    )
    in_before, in_after = from_sides(coarse_in, coarse_in)
    mine, slope = lax.optimization_barrier((mine, slope))
    other = lax.ppermute(mine, "gz", [(i, i ^ 1) for i in range(slabs)])
    coarse_grad, features, packed = call(
        coarse_forward,
        [((64, 128), BF16), ((128, 128), BF16), ((128, 3456), BF16)],
        coarse_in, in_before, in_after, mine, other,
        scratch=[((128, 128), F32)],
        core=core,
    )
    grad_before, grad_after = from_sides(coarse_grad, coarse_grad)
    parts, fine_grad = call(
        backward,
        [((group, 168, 128), BF16), ((2, 128, 128), BF16)],
        coarse_grad, grad_before, grad_after, packed, pooled, slope, windows, down_kernel,
        coarse_in, features,
        scratch=[((256, 128), F32), ((1408, 128), F32)],
    )
    parts = exchange(parts, "grp")
    fine_before, fine_after = from_sides(fine_grad[1], fine_grad[0])
    (volume_grad,) = call(
        fine_backward,
        [((2, 16, 1024), BF16)],
        fine_grad, fine_before, fine_after, behind,
        scratch=[((4, 128, 256), BF16)],
        far=(0,),
    )
    parts, volume_grad = lax.optimization_barrier((parts, volume_grad))
    out_rows, terms = call(
        coarse_kernel_terms,
        [((group, 8, 64), BF16), ((slabs, 16, 128), BF16)],
        parts,
        scratch=[((72, 1024), F32), ((1024, 384), BF16)],
        far=(0,),
    )
    terms = exchange(terms, "gz")
    (terms,) = call(sum_slabs, [((slabs, 16, 128), BF16)], terms)
    terms = exchange(terms, "gz")
    coarse_kg, shared = call(collect, [((8, 3456), F32), ((group, 88, 128), BF16)], terms, far=(0,))
    shared = exchange(shared, "grp").reshape(1408, 128)
    fine_kg, down_kg = call(unpack, [((64, 1728), F32), ((512, 128), F32)], shared, far=(0, 1))
    coarse_out = jnp.swapaxes(out_rows, 1, 2)[:, None]
    return (coarse_out, volume_grad[None], fine_kg.T, down_kg, coarse_kg.T)


def solution(mesh):
    in_specs = (P("grp", "gz", None, None), P(None, "gz", None, "grp"), P(), P(), P(None, "grp"))
    out_specs = (P(None, "gz", None, "grp"), P("grp", "gz", None, None), P(), P(), P(None, "grp"))
    return jax.shard_map(
        per_device, mesh=mesh, in_specs=in_specs, out_specs=out_specs, check_vma=False
    )
```

```python
import jax
import jax.numpy as jnp
from jax import lax
from jax.experimental import pallas as pl
from jax.experimental.pallas import tpu as pltpu
from jax.sharding import PartitionSpec as P


F32 = jnp.float32
BF16 = jnp.bfloat16
NN = (((1,), (0,)), ((), ()))
NT = (((1,), (1,)), ((), ()))
TN = (((0,), (0,)), ((), ()))


def mm(left, right, dims):
    return lax.dot_general(left, right, dims, preferred_element_type=F32)


def shift_rows(value, by, period):
    total = value.shape[0]
    place = lax.broadcasted_iota(jnp.int32, value.shape, 0) % period
    inside = place != (0 if by == 1 else period - 1)
    return jnp.where(inside, pltpu.roll(value, by % total, 0), 0.0)


def low_half(rows):
    return lax.broadcasted_iota(jnp.int32, (rows, 128), 1) < 64


def slope_and_silu(pre):
    sig = jax.nn.sigmoid(pre)
    return sig * (1.0 + pre * (1.0 - sig)), pre * sig


def fill_windows(windows, plane, blocks):
    low = low_half(16)
    none = jnp.zeros((16, 128), BF16)
    for j in range(8):
        after = blocks[j + 1] if j < 7 else none
        before = blocks[j - 1] if j > 0 else none
        rows = pl.ds(j * 16, 16)
        windows[plane, rows, 0:128] = blocks[j]
        windows[plane, rows, 128:256] = jnp.where(low, after, before)


def window_conv(windows, weights, dims):
    parts = []
    for dx in range(3):
        total = None
        for dz in range(3):
            rows = windows[dz : dz + 2].reshape(256, 256)
            term = mm(rows, weights[dz * 3 + dx], dims)
            total = term if total is None else total + term
        parts.append(total)
    return parts[1] + shift_rows(parts[0], 1, 16) + shift_rows(parts[2], -1, 16)


def place_weights(kernel, ahead, behind):
    low = low_half(64)
    tiles = [kernel[:, m * 128 : (m + 1) * 128].astype(F32) for m in range(13)]
    last = kernel[:, 1664:1728].astype(F32)
    tiles.append(jnp.concatenate([last, jnp.zeros((64, 64), F32)], axis=1))
    for k in range(9):
        first, second = tiles[3 * k // 2], tiles[3 * k // 2 + 1]
        swapped = pltpu.roll(jnp.where(low, second, first), 64, 1)
        if k % 2 == 0:
            zero_one, two_none = first, jnp.where(low, second, 0.0)
            one_two, none_zero = swapped, pltpu.roll(jnp.where(low, first, 0.0), 64, 1)
        else:
            one_two, none_zero = second, jnp.where(low, 0.0, first)
            zero_one, two_none = swapped, pltpu.roll(jnp.where(low, 0.0, second), 64, 1)
        blocks = [part.astype(BF16) for part in (one_two, zero_one, none_zero, two_none)]
        ahead[k, 0:64, 0:128] = blocks[0]
        ahead[k, 64:128, 0:128] = blocks[1]
        ahead[k, 0:64, 128:256] = blocks[2]
        ahead[k, 64:128, 128:256] = blocks[3]
        for slot in range(4):
            behind[8 - k, slot * 64 : (slot + 1) * 64] = blocks[slot]


def sort_sides(core, near, far, sides):
    @pl.when(core[0] == 0)
    def _():
        sides[0] = far[...]
        sides[1] = near[...]

    @pl.when(core[0] == 1)
    def _():
        sides[0] = near[...]
        sides[1] = far[...]


def fine_forward(
    core, vol, near, far, weights, down, coarse, slope, windows, pooled, act, sides
):
    sort_sides(core, near, far, sides)

    def lanes(side, j):
        return sides[side, :, j * 128 : (j + 1) * 128]

    fill_windows(windows, 0, [lanes(0, j) for j in range(8)])
    fill_windows(windows, 1, [vol[0, :, j * 128 : (j + 1) * 128] for j in range(8)])
    fill_windows(windows, 2, [vol[1, :, j * 128 : (j + 1) * 128] for j in range(8)])
    fill_windows(windows, 3, [lanes(1, j) for j in range(8)])
    pre = window_conv(windows, weights, NT)
    slopes, silu = slope_and_silu(pre)
    slope[...] = slopes
    act[...] = silu
    for z in range(2):
        for bx in range(2):
            part = act[pl.ds(z * 128 + bx, 64, stride=2), :]
            at = (z * 2 + bx) * 128
            pooled[:, at : at + 128] = part.astype(BF16)
    coarse[...] = mm(pooled[...], down[...], NN).astype(BF16)


def y_taps(plane):
    value = plane[...].astype(F32)
    edge = jnp.zeros((8, 128), F32)
    earlier = jnp.concatenate([edge, value[:-8]], axis=0)
    later = jnp.concatenate([value[8:], edge], axis=0)
    return jnp.concatenate([earlier, value, later], axis=1).astype(BF16)


HALF = 1792


def spread_half(core, kernel, cotangent, out):
    for at in range(16):
        tail = jnp.concatenate([cotangent[at].astype(F32), jnp.zeros((8, 64), F32)], axis=1)
        out[at, :, HALF : HALF + 128] = tail.astype(BF16)

    @pl.when(core[0] == 0)
    def _():
        for at in range(16):
            out[at, :, 0:HALF] = kernel[:, 0:HALF]

    @pl.when(core[0] == 1)
    def _():
        for at in range(16):
            out[at, :, 0:HALF] = kernel[:, 3456 - HALF : 3456]


def coarse_forward(core, own, near, far, mine, other, grad, out, packed, scratch, sides):
    sort_sides(core, near, far, sides)
    before, after = sides.at[0], sides.at[1]
    rest = 3456 - HALF

    @pl.when(core[0] == 0)
    def _():
        packed[:, 0:HALF] = mine[:, 0:HALF]
        packed[:, HALF:3456] = other[:, HALF - rest : HALF]

    @pl.when(core[0] == 1)
    def _():
        packed[:, 0:rest] = other[:, 0:rest]
        packed[:, rest:3456] = mine[:, 0:HALF]

    planes = [y_taps(before), y_taps(own), y_taps(after)]
    parts = []
    for dx in range(3):
        total = None
        for dz in range(3):
            at = (dz * 3 + dx) * 384
            term = mm(planes[dz], packed[:, at : at + 384], NT)
            total = term if total is None else total + term
        parts.append(total)
    pre = parts[1] + shift_rows(parts[0], 1, 8) + shift_rows(parts[2], -1, 8)
    slopes, silu = slope_and_silu(pre)
    scratch[0:64] = silu
    by_x = [scratch[pl.ds(x, 8, stride=8), :] for x in range(8)]
    scratch[...] = mine[:, HALF : HALF + 128].astype(F32).T
    cotangent = jnp.concatenate([scratch[pl.ds(y, 8, stride=8), :] for y in range(8)], axis=0)
    slopes = (cotangent * slopes).astype(BF16)
    grad[...] = slopes
    out[...] = jnp.concatenate(by_x + [slopes.astype(F32)], axis=0).T.astype(BF16)


def coarse_kernel_terms(parts, features, terms, grads, taps):
    low = low_half(8)
    place = lax.broadcasted_iota(jnp.int32, (8, 128), 1) % 8
    for volume in range(16):
        taps[volume * 64 : (volume + 1) * 64] = y_taps(parts[volume, 0:64])
        features[volume] = parts[volume, 64:72, 0:64]
    for pair in range(8):
        first = parts[pair * 2, 64:80].astype(F32)
        second = parts[pair * 2 + 1, 64:80].astype(F32)
        own = jnp.where(low, pltpu.roll(first[0:8], 64, 1), second[0:8])
        before = jnp.where(low, first[8:16], pltpu.roll(second[8:16], 64, 1))
        after = jnp.where(low, pltpu.roll(first[8:16], 64, 1), second[8:16])
        for dz, value in enumerate((after, own, before)):
            earlier = jnp.where(place != 7, pltpu.roll(value, 127, 1), 0.0)
            later = jnp.where(place != 0, pltpu.roll(value, 1, 1), 0.0)
            for dx, moved in enumerate((earlier, value, later)):
                at = (dz * 3 + dx) * 8
                grads[at : at + 8, pair * 128 : (pair + 1) * 128] = moved
    total = mm(grads[...].astype(BF16), taps[...], NN)
    shared = []
    for at in range(80, 160, 16):
        both = jnp.sum(parts[:, at : at + 16, :].astype(F32), axis=0)
        shared += [both[0:8], both[8:16]]
    shared.append(jnp.sum(parts[:, 160:168, :].astype(F32), axis=0))
    none = jnp.zeros((8, 128), F32)
    for device in range(32):
        k, dy = divmod(device, 3)
        own = total[k * 8 : k * 8 + 8, dy * 128 : (dy + 1) * 128] if device < 27 else none
        other = shared[device] if device < 11 else none
        terms[device] = jnp.concatenate([own, other], axis=0).astype(BF16)


def backward(
    core, own, near, far, packed, pooled, slope, windows, down, coarse_in, features,
    out, fine_grad, act, shared, sides,
):
    sort_sides(core, near, far, sides)
    before, after = sides.at[0], sides.at[1]
    planes = [after[...], own[...], before[...]]
    edge = jnp.zeros((8, 128), F32)
    parts = []
    for dx in range(3):
        total = None
        for dz in range(3):
            at = (dz * 3 + dx) * 384
            term = mm(planes[dz], packed[:, at : at + 384], NN)
            total = term if total is None else total + term
        earlier = jnp.concatenate([total[8:, 0:128], edge], axis=0)
        later = jnp.concatenate([edge, total[:-8, 256:384]], axis=0)
        parts.append(earlier + total[:, 128:256] + later)
    in_grad = parts[1] + shift_rows(parts[0], -1, 8) + shift_rows(parts[2], 1, 8)
    in_grad = in_grad.astype(BF16)
    act_grad = mm(in_grad, down[...], NT)
    for z in range(2):
        for bx in range(2):
            at = (z * 2 + bx) * 128
            act[pl.ds(z * 128 + bx, 64, stride=2), :] = act_grad[:, at : at + 128]
    grad = (act[...] * slope[...]).astype(BF16)
    fine_grad[0] = grad[0:128]
    fine_grad[1] = grad[128:256]
    value = grad.astype(F32)
    moved = [shift_rows(value, -1, 16), value, shift_rows(value, 1, 16)]
    moved = [part.astype(BF16) for part in moved]
    low = low_half(64)
    held = None
    for dz in range(3):
        rows = windows[dz : dz + 2].reshape(256, 256)
        for dx in range(3):
            block = mm(moved[dx], rows, TN)
            u0, u1 = block[0:64, 0:128], block[0:64, 128:256]
            v0, v1 = block[64:128, 0:128], block[64:128, 128:256]
            for dy, (left, right) in enumerate(((u1, v0), (v0, u0), (u0, v1))):
                tap = (dz * 3 + dx) * 3 + dy
                if tap % 2 == 0:
                    held = pltpu.roll(left, 64, 1) + right
                else:
                    high = left + pltpu.roll(right, 64, 1)
                    at = (tap // 2) * 64
                    shared[at : at + 64] = jnp.where(low, held, high)
    shared[832:896] = jnp.where(low, held, 0.0)
    shared[896:1408] = mm(pooled[...], in_grad, TN)
    sides = jnp.concatenate([before[...].astype(F32), after[...].astype(F32)], axis=0).T
    for at in range(16):
        rows = slice(at * 8, at * 8 + 8)
        out[at, 0:64] = coarse_in[...]
        mixed = jnp.concatenate([features[rows].astype(F32), sides[rows]], axis=0)
        out[at, 64:80] = mixed.astype(BF16)
        out[at, 80:168] = shared[at * 88 : at * 88 + 88].astype(BF16)


def fine_backward(grad, before, after, weights, out, windows):
    def blocks(plane):
        return [plane[j * 16 : (j + 1) * 16] for j in range(8)]

    fill_windows(windows, 0, blocks(before[...]))
    fill_windows(windows, 1, blocks(grad[0]))
    fill_windows(windows, 2, blocks(grad[1]))
    fill_windows(windows, 3, blocks(after[...]))
    total = window_conv(windows, weights, NN).astype(BF16)
    for z in range(2):
        for j in range(8):
            at = z * 128 + j * 16
            out[z, :, j * 128 : (j + 1) * 128] = total[at : at + 16]


def sum_slabs(terms, out):
    total = jnp.sum(terms[...].astype(F32), axis=0).astype(BF16)
    for device in range(32):
        out[device] = total


def collect(terms, coarse, out):
    rows = []
    for device in range(27):
        both = terms[device].astype(F32)
        coarse[:, device * 128 : (device + 1) * 128] = both[0:8]
        rows.append(both[8:16])
    total = jnp.concatenate(rows[0:11], axis=0).astype(BF16)
    for device in range(16):
        out[device] = total


def unpack(shared, fine, down):
    for tile in range(13):
        rows = shared[tile * 64 : (tile + 1) * 64]
        fine[:, tile * 128 : (tile + 1) * 128] = rows.astype(F32)
    fine[:, 1664:1728] = shared[832:896].astype(F32)[:, 0:64]
    down[...] = shared[896:1408].astype(F32)


def call(body, outs, *operands, scratch=(), far=(), core=None, moved=True):
    place = [jax.ShapeDtypeStruct if at in far else pltpu.VMEM for at in range(len(outs))]
    first = [] if core is None else [core]
    if moved:
        operands = [pltpu.with_memory_space_constraint(part, pltpu.VMEM) for part in operands]
    specs = [pl.BlockSpec(memory_space=pltpu.SMEM) for _ in first]
    return pl.pallas_call(
        body,
        out_shape=[put(*out) for put, out in zip(place, outs)],
        in_specs=specs + [pl.BlockSpec(memory_space=pltpu.VMEM) for _ in operands],
        scratch_shapes=[pltpu.VMEM(shape, kind) for shape, kind in scratch],
        cost_estimate=pl.CostEstimate(flops=WORK, transcendentals=0, bytes_accessed=1 << 20),
        interpret=INTERPRET,
    )(*first, *operands)


INTERPRET = False
WORK = 250_000_000


def from_sides(last, first):
    devices = lax.axis_size("gz")
    up = [(i, i + 1) for i in range(devices - 1)]
    down = [(j, i) for i, j in up]
    return lax.ppermute(last, "gz", up), lax.ppermute(first, "gz", down)


def pair_swaps(to_core, to_other):
    devices = lax.axis_size("gz")
    up = [(i, i + 1) for i in range(1, devices - 1, 2)]
    near = lax.ppermute(to_core, "gz", [(i, i ^ 1) for i in range(devices)])
    far = lax.ppermute(to_other, "gz", up + [(j, i) for i, j in up])
    return near, far


def exchange(blocks, axis):
    return lax.all_to_all(blocks, axis, 0, 0, tiled=True)


def per_device(volumes, cotangent, fine_kernel, down_kernel, coarse_kernel):
    group = lax.axis_size("grp")
    slabs = lax.axis_size("gz")
    vol = volumes[0]
    core = (lax.axis_index("gz") & 1).astype(jnp.int32).reshape(1)
    (halves,) = call(
        spread_half,
        [((group, 8, HALF + 128), BF16)],
        coarse_kernel.T, jnp.swapaxes(cotangent[:, 0], 1, 2),
        core=core,
        moved=False,
    )
    index = core[0]
    near, far = pair_swaps(
        lax.dynamic_index_in_dim(vol, 1 - index, 0, keepdims=False),
        lax.dynamic_index_in_dim(vol, index, 0, keepdims=False),
    )
    mine = exchange(halves, "grp").reshape(128, HALF + 128)
    ahead, behind = call(
        place_weights, [((9, 128, 256), BF16), ((9, 256, 128), BF16)], fine_kernel.T, far=(1,)
    )

    coarse_in, slope, windows, pooled = call(
        fine_forward,
        [((64, 128), BF16), ((256, 128), F32), ((4, 128, 256), BF16), ((64, 512), BF16)],
        vol, near, far, ahead, down_kernel,
        scratch=[((256, 128), F32), ((2, 16, 1024), BF16)],
        core=core,
        far=(2,),
    )
    in_near, in_far = pair_swaps(coarse_in, coarse_in)
    mine, slope = lax.optimization_barrier((mine, slope))
    other = lax.ppermute(mine, "gz", [(i, i ^ 1) for i in range(slabs)])
    coarse_grad, features, packed = call(
        coarse_forward,
        [((64, 128), BF16), ((128, 128), BF16), ((128, 3456), BF16)],
        coarse_in, in_near, in_far, mine, other,
        scratch=[((128, 128), F32), ((2, 64, 128), BF16)],
        core=core,
    )
    grad_near, grad_far = pair_swaps(coarse_grad, coarse_grad)
    parts, fine_grad = call(
        backward,
        [((group, 168, 128), BF16), ((2, 128, 128), BF16)],
        coarse_grad, grad_near, grad_far, packed, pooled, slope, windows, down_kernel,
        coarse_in, features,
        scratch=[((256, 128), F32), ((1408, 128), F32), ((2, 64, 128), BF16)],
        core=core,
    )
    parts = exchange(parts, "grp")
    fine_before, fine_after = from_sides(fine_grad[1], fine_grad[0])
    (volume_grad,) = call(
        fine_backward,
        [((2, 16, 1024), BF16)],
        fine_grad, fine_before, fine_after, behind,
        scratch=[((4, 128, 256), BF16)],
        far=(0,),
    )
    parts, volume_grad = lax.optimization_barrier((parts, volume_grad))
    out_rows, terms = call(
        coarse_kernel_terms,
        [((group, 8, 64), BF16), ((slabs, 16, 128), BF16)],
        parts,
        scratch=[((72, 1024), F32), ((1024, 384), BF16)],
        far=(0,),
    )
    terms = exchange(terms, "gz")
    (terms,) = call(sum_slabs, [((slabs, 16, 128), BF16)], terms)
    terms = exchange(terms, "gz")
    coarse_kg, shared = call(collect, [((8, 3456), F32), ((group, 88, 128), BF16)], terms, far=(0,))
    shared = exchange(shared, "grp").reshape(1408, 128)
    fine_kg, down_kg = call(unpack, [((64, 1728), F32), ((512, 128), F32)], shared, far=(0, 1))
    coarse_out = jnp.swapaxes(out_rows, 1, 2)[:, None]
    return (coarse_out, volume_grad[None], fine_kg.T, down_kg, coarse_kg.T)


def solution(mesh):
    in_specs = (P("grp", "gz", None, None), P(None, "gz", None, "grp"), P(), P(), P(None, "grp"))
    out_specs = (P(None, "gz", None, "grp"), P("grp", "gz", None, None), P(), P(), P(None, "grp"))
    return jax.shard_map(
        per_device, mesh=mesh, in_specs=in_specs, out_specs=out_specs, check_vma=False
    )
```

```python
import jax
import jax.numpy as jnp
from jax import lax
from jax.experimental import pallas as pl
from jax.experimental.pallas import tpu as pltpu
from jax.sharding import PartitionSpec as P


F32 = jnp.float32
BF16 = jnp.bfloat16
NN = (((1,), (0,)), ((), ()))
NT = (((1,), (1,)), ((), ()))
TN = (((0,), (0,)), ((), ()))


def mm(left, right, dims):
    return lax.dot_general(left, right, dims, preferred_element_type=F32)


def shift_rows(value, by, period):
    total = value.shape[0]
    place = lax.broadcasted_iota(jnp.int32, value.shape, 0) % period
    inside = place != (0 if by == 1 else period - 1)
    return jnp.where(inside, pltpu.roll(value, by % total, 0), 0.0)


def low_half(rows):
    return lax.broadcasted_iota(jnp.int32, (rows, 128), 1) < 64


def slope_and_silu(pre):
    sig = jax.nn.sigmoid(pre)
    return sig * (1.0 + pre * (1.0 - sig)), pre * sig


def fill_windows(windows, plane, blocks):
    low = low_half(16)
    none = jnp.zeros((16, 128), BF16)
    for j in range(8):
        after = blocks[j + 1] if j < 7 else none
        before = blocks[j - 1] if j > 0 else none
        rows = pl.ds(j * 16, 16)
        windows[plane, rows, 0:128] = blocks[j]
        windows[plane, rows, 128:256] = jnp.where(low, after, before)


def window_conv(windows, weights, dims):
    parts = []
    for dx in range(3):
        total = None
        for dz in range(3):
            rows = windows[dz : dz + 2].reshape(256, 256)
            term = mm(rows, weights[dz * 3 + dx], dims)
            total = term if total is None else total + term
        parts.append(total)
    return parts[1] + shift_rows(parts[0], 1, 16) + shift_rows(parts[2], -1, 16)


def place_weights(kernel, ahead, behind):
    low = low_half(64)
    tiles = [kernel[:, m * 128 : (m + 1) * 128].astype(F32) for m in range(13)]
    last = kernel[:, 1664:1728].astype(F32)
    tiles.append(jnp.concatenate([last, jnp.zeros((64, 64), F32)], axis=1))
    for k in range(9):
        first, second = tiles[3 * k // 2], tiles[3 * k // 2 + 1]
        swapped = pltpu.roll(jnp.where(low, second, first), 64, 1)
        if k % 2 == 0:
            zero_one, two_none = first, jnp.where(low, second, 0.0)
            one_two, none_zero = swapped, pltpu.roll(jnp.where(low, first, 0.0), 64, 1)
        else:
            one_two, none_zero = second, jnp.where(low, 0.0, first)
            zero_one, two_none = swapped, pltpu.roll(jnp.where(low, 0.0, second), 64, 1)
        blocks = [part.astype(BF16) for part in (one_two, zero_one, none_zero, two_none)]
        ahead[k, 0:64, 0:128] = blocks[0]
        ahead[k, 64:128, 0:128] = blocks[1]
        ahead[k, 0:64, 128:256] = blocks[2]
        ahead[k, 64:128, 128:256] = blocks[3]
        for slot in range(4):
            behind[8 - k, slot * 64 : (slot + 1) * 64] = blocks[slot]


def sort_sides(core, near, far, sides):
    @pl.when(core[0] == 0)
    def _():
        sides[0] = far[...]
        sides[1] = near[...]

    @pl.when(core[0] == 1)
    def _():
        sides[0] = near[...]
        sides[1] = far[...]


def fine_forward(
    core, vol, near, far, weights, down, coarse, slope, windows, pooled, act, sides
):
    sort_sides(core, near, far, sides)

    def lanes(side, j):
        return sides[side, :, j * 128 : (j + 1) * 128]

    fill_windows(windows, 0, [lanes(0, j) for j in range(8)])
    fill_windows(windows, 1, [vol[0, :, j * 128 : (j + 1) * 128] for j in range(8)])
    fill_windows(windows, 2, [vol[1, :, j * 128 : (j + 1) * 128] for j in range(8)])
    fill_windows(windows, 3, [lanes(1, j) for j in range(8)])
    pre = window_conv(windows, weights, NT)
    slopes, silu = slope_and_silu(pre)
    slope[...] = slopes
    act[...] = silu
    for z in range(2):
        for bx in range(2):
            part = act[pl.ds(z * 128 + bx, 64, stride=2), :]
            at = (z * 2 + bx) * 128
            pooled[:, at : at + 128] = part.astype(BF16)
    coarse[...] = mm(pooled[...], down[...], NN).astype(BF16)


def y_taps(plane):
    value = plane[...].astype(F32)
    edge = jnp.zeros((8, 128), F32)
    earlier = jnp.concatenate([edge, value[:-8]], axis=0)
    later = jnp.concatenate([value[8:], edge], axis=0)
    return jnp.concatenate([earlier, value, later], axis=1).astype(BF16)


HALF = 1792


def spread_half(core, kernel, cotangent, out):
    for at in range(16):
        tail = jnp.concatenate([cotangent[at].astype(F32), jnp.zeros((8, 64), F32)], axis=1)
        out[at, :, HALF : HALF + 128] = tail.astype(BF16)

    @pl.when(core[0] == 0)
    def _():
        for at in range(16):
            out[at, :, 0:HALF] = kernel[:, 0:HALF]

    @pl.when(core[0] == 1)
    def _():
        for at in range(16):
            out[at, :, 0:HALF] = kernel[:, 3456 - HALF : 3456]


def insert_plane(mine, coarse_in, out):
    out[:, 0:HALF] = mine[:, 0:HALF]
    cotangent = mine[:, HALF : HALF + 128].astype(F32)[:, 0:64]
    plane = coarse_in[...].astype(F32).T
    out[:, HALF : HALF + 128] = jnp.concatenate([cotangent, plane], axis=1).astype(BF16)


def coarse_forward(
    core, own, far, mine, other, grad, out, packed, scratch, sides, near
):
    near[...] = other[:, HALF : HALF + 128].astype(F32).T[64:128].astype(BF16)
    sort_sides(core, near, far, sides)
    before, after = sides.at[0], sides.at[1]
    rest = 3456 - HALF

    @pl.when(core[0] == 0)
    def _():
        packed[:, 0:HALF] = mine[:, 0:HALF]
        packed[:, HALF:3456] = other[:, HALF - rest : HALF]

    @pl.when(core[0] == 1)
    def _():
        packed[:, 0:rest] = other[:, 0:rest]
        packed[:, rest:3456] = mine[:, 0:HALF]

    planes = [y_taps(before), y_taps(own), y_taps(after)]
    parts = []
    for dx in range(3):
        total = None
        for dz in range(3):
            at = (dz * 3 + dx) * 384
            term = mm(planes[dz], packed[:, at : at + 384], NT)
            total = term if total is None else total + term
        parts.append(total)
    pre = parts[1] + shift_rows(parts[0], 1, 8) + shift_rows(parts[2], -1, 8)
    slopes, silu = slope_and_silu(pre)
    scratch[0:64] = silu
    by_x = [scratch[pl.ds(x, 8, stride=8), :] for x in range(8)]
    scratch[...] = mine[:, HALF : HALF + 128].astype(F32).T
    cotangent = jnp.concatenate([scratch[pl.ds(y, 8, stride=8), :] for y in range(8)], axis=0)
    slopes = (cotangent * slopes).astype(BF16)
    grad[...] = slopes
    out[...] = jnp.concatenate(by_x + [slopes.astype(F32)], axis=0).T.astype(BF16)


def coarse_kernel_terms(parts, features, terms, grads, taps):
    low = low_half(8)
    place = lax.broadcasted_iota(jnp.int32, (8, 128), 1) % 8
    for volume in range(16):
        taps[volume * 64 : (volume + 1) * 64] = y_taps(parts[volume, 0:64])
        features[volume] = parts[volume, 64:72, 0:64]
    for pair in range(8):
        first = parts[pair * 2, 64:80].astype(F32)
        second = parts[pair * 2 + 1, 64:80].astype(F32)
        own = jnp.where(low, pltpu.roll(first[0:8], 64, 1), second[0:8])
        before = jnp.where(low, first[8:16], pltpu.roll(second[8:16], 64, 1))
        after = jnp.where(low, pltpu.roll(first[8:16], 64, 1), second[8:16])
        for dz, value in enumerate((after, own, before)):
            earlier = jnp.where(place != 7, pltpu.roll(value, 127, 1), 0.0)
            later = jnp.where(place != 0, pltpu.roll(value, 1, 1), 0.0)
            for dx, moved in enumerate((earlier, value, later)):
                at = (dz * 3 + dx) * 8
                grads[at : at + 8, pair * 128 : (pair + 1) * 128] = moved
    total = mm(grads[...].astype(BF16), taps[...], NN)
    shared = []
    for at in range(80, 160, 16):
        both = jnp.sum(parts[:, at : at + 16, :].astype(F32), axis=0)
        shared += [both[0:8], both[8:16]]
    shared.append(jnp.sum(parts[:, 160:168, :].astype(F32), axis=0))
    none = jnp.zeros((8, 128), F32)
    for device in range(32):
        k, dy = divmod(device, 3)
        own = total[k * 8 : k * 8 + 8, dy * 128 : (dy + 1) * 128] if device < 27 else none
        other = shared[device] if device < 11 else none
        terms[device] = jnp.concatenate([own, other], axis=0).astype(BF16)


def backward(
    core, own, near, far, packed, pooled, slope, windows, down, coarse_in, features,
    out, fine_grad, act, shared, sides,
):
    sort_sides(core, near, far, sides)
    before, after = sides.at[0], sides.at[1]
    planes = [after[...], own[...], before[...]]
    edge = jnp.zeros((8, 128), F32)
    parts = []
    for dx in range(3):
        total = None
        for dz in range(3):
            at = (dz * 3 + dx) * 384
            term = mm(planes[dz], packed[:, at : at + 384], NN)
            total = term if total is None else total + term
        earlier = jnp.concatenate([total[8:, 0:128], edge], axis=0)
        later = jnp.concatenate([edge, total[:-8, 256:384]], axis=0)
        parts.append(earlier + total[:, 128:256] + later)
    in_grad = parts[1] + shift_rows(parts[0], -1, 8) + shift_rows(parts[2], 1, 8)
    in_grad = in_grad.astype(BF16)
    act_grad = mm(in_grad, down[...], NT)
    for z in range(2):
        for bx in range(2):
            at = (z * 2 + bx) * 128
            act[pl.ds(z * 128 + bx, 64, stride=2), :] = act_grad[:, at : at + 128]
    grad = (act[...] * slope[...]).astype(BF16)
    fine_grad[0] = grad[0:128]
    fine_grad[1] = grad[128:256]
    value = grad.astype(F32)
    moved = [shift_rows(value, -1, 16), value, shift_rows(value, 1, 16)]
    moved = [part.astype(BF16) for part in moved]
    low = low_half(64)
    held = None
    for dz in range(3):
        rows = windows[dz : dz + 2].reshape(256, 256)
        for dx in range(3):
            block = mm(moved[dx], rows, TN)
            u0, u1 = block[0:64, 0:128], block[0:64, 128:256]
            v0, v1 = block[64:128, 0:128], block[64:128, 128:256]
            for dy, (left, right) in enumerate(((u1, v0), (v0, u0), (u0, v1))):
                tap = (dz * 3 + dx) * 3 + dy
                if tap % 2 == 0:
                    held = pltpu.roll(left, 64, 1) + right
                else:
                    high = left + pltpu.roll(right, 64, 1)
                    at = (tap // 2) * 64
                    shared[at : at + 64] = jnp.where(low, held, high)
    shared[832:896] = jnp.where(low, held, 0.0)
    shared[896:1408] = mm(pooled[...], in_grad, TN)
    sides = jnp.concatenate([before[...].astype(F32), after[...].astype(F32)], axis=0).T
    for at in range(16):
        rows = slice(at * 8, at * 8 + 8)
        out[at, 0:64] = coarse_in[...]
        mixed = jnp.concatenate([features[rows].astype(F32), sides[rows]], axis=0)
        out[at, 64:80] = mixed.astype(BF16)
        out[at, 80:168] = shared[at * 88 : at * 88 + 88].astype(BF16)


def fine_backward(grad, before, after, weights, out, windows):
    def blocks(plane):
        return [plane[j * 16 : (j + 1) * 16] for j in range(8)]

    fill_windows(windows, 0, blocks(before[...]))
    fill_windows(windows, 1, blocks(grad[0]))
    fill_windows(windows, 2, blocks(grad[1]))
    fill_windows(windows, 3, blocks(after[...]))
    total = window_conv(windows, weights, NN).astype(BF16)
    for z in range(2):
        for j in range(8):
            at = z * 128 + j * 16
            out[z, :, j * 128 : (j + 1) * 128] = total[at : at + 16]


def sum_slabs(terms, out):
    total = jnp.sum(terms[...].astype(F32), axis=0).astype(BF16)
    for device in range(32):
        out[device] = total


def collect(terms, coarse, out):
    rows = []
    for device in range(27):
        both = terms[device].astype(F32)
        coarse[:, device * 128 : (device + 1) * 128] = both[0:8]
        rows.append(both[8:16])
    total = jnp.concatenate(rows[0:11], axis=0).astype(BF16)
    for device in range(16):
        out[device] = total


def unpack(shared, fine, down):
    for tile in range(13):
        rows = shared[tile * 64 : (tile + 1) * 64]
        fine[:, tile * 128 : (tile + 1) * 128] = rows.astype(F32)
    fine[:, 1664:1728] = shared[832:896].astype(F32)[:, 0:64]
    down[...] = shared[896:1408].astype(F32)


def call(body, outs, *operands, scratch=(), far=(), core=None, moved=True):
    place = [jax.ShapeDtypeStruct if at in far else pltpu.VMEM for at in range(len(outs))]
    first = [] if core is None else [core]
    if moved:
        operands = [pltpu.with_memory_space_constraint(part, pltpu.VMEM) for part in operands]
    specs = [pl.BlockSpec(memory_space=pltpu.SMEM) for _ in first]
    return pl.pallas_call(
        body,
        out_shape=[put(*out) for put, out in zip(place, outs)],
        in_specs=specs + [pl.BlockSpec(memory_space=pltpu.VMEM) for _ in operands],
        scratch_shapes=[pltpu.VMEM(shape, kind) for shape, kind in scratch],
        cost_estimate=pl.CostEstimate(flops=WORK, transcendentals=0, bytes_accessed=1 << 20),
        interpret=INTERPRET,
    )(*first, *operands)


INTERPRET = False
WORK = 250_000_000


def from_sides(last, first):
    devices = lax.axis_size("gz")
    up = [(i, i + 1) for i in range(devices - 1)]
    down = [(j, i) for i, j in up]
    return lax.ppermute(last, "gz", up), lax.ppermute(first, "gz", down)


def core_swap(array):
    return lax.ppermute(array, "gz", [(i, i ^ 1) for i in range(lax.axis_size("gz"))])


def other_swap(array):
    up = [(i, i + 1) for i in range(1, lax.axis_size("gz") - 1, 2)]
    return lax.ppermute(array, "gz", up + [(j, i) for i, j in up])


def pair_swaps(to_core, to_other):
    return core_swap(to_core), other_swap(to_other)


def exchange(blocks, axis):
    return lax.all_to_all(blocks, axis, 0, 0, tiled=True)


def per_device(volumes, cotangent, fine_kernel, down_kernel, coarse_kernel):
    group = lax.axis_size("grp")
    slabs = lax.axis_size("gz")
    vol = volumes[0]
    core = (lax.axis_index("gz") & 1).astype(jnp.int32).reshape(1)
    (halves,) = call(
        spread_half,
        [((group, 8, HALF + 128), BF16)],
        coarse_kernel.T, jnp.swapaxes(cotangent[:, 0], 1, 2),
        core=core,
        moved=False,
    )
    index = core[0]
    near, far = pair_swaps(
        lax.dynamic_index_in_dim(vol, 1 - index, 0, keepdims=False),
        lax.dynamic_index_in_dim(vol, index, 0, keepdims=False),
    )
    mine = exchange(halves, "grp").reshape(128, HALF + 128)
    ahead, behind = call(
        place_weights, [((9, 128, 256), BF16), ((9, 256, 128), BF16)], fine_kernel.T, far=(1,)
    )

    coarse_in, slope, windows, pooled = call(
        fine_forward,
        [((64, 128), BF16), ((256, 128), F32), ((4, 128, 256), BF16), ((64, 512), BF16)],
        vol, near, far, ahead, down_kernel,
        scratch=[((256, 128), F32), ((2, 16, 1024), BF16)],
        core=core,
        far=(1, 2),
    )
    in_far = other_swap(coarse_in)
    (mine,) = call(insert_plane, [((128, HALF + 128), BF16)], mine, coarse_in)
    other = core_swap(mine)
    coarse_grad, features, packed = call(
        coarse_forward,
        [((64, 128), BF16), ((128, 128), BF16), ((128, 3456), BF16)],
        coarse_in, in_far, mine, other,
        scratch=[((128, 128), F32), ((2, 64, 128), BF16), ((64, 128), BF16)],
        core=core,
    )
    grad_near, grad_far = pair_swaps(coarse_grad, coarse_grad)
    parts, fine_grad = call(
        backward,
        [((group, 168, 128), BF16), ((2, 128, 128), BF16)],
        coarse_grad, grad_near, grad_far, packed, pooled, slope, windows, down_kernel,
        coarse_in, features,
        scratch=[((256, 128), F32), ((1408, 128), F32), ((2, 64, 128), BF16)],
        core=core,
    )
    parts = exchange(parts, "grp")
    out_rows, terms = call(
        coarse_kernel_terms,
        [((group, 8, 64), BF16), ((slabs, 16, 128), BF16)],
        parts,
        scratch=[((72, 1024), F32), ((1024, 384), BF16)],
        far=(0,),
    )
    terms = exchange(terms, "gz")
    (terms,) = call(sum_slabs, [((slabs, 16, 128), BF16)], terms)
    terms = exchange(terms, "gz")
    fine_before, fine_after = from_sides(fine_grad[1], fine_grad[0])
    (volume_grad,) = call(
        fine_backward,
        [((2, 16, 1024), BF16)],
        fine_grad, fine_before, fine_after, behind,
        scratch=[((4, 128, 256), BF16)],
        far=(0,),
    )
    terms, volume_grad = lax.optimization_barrier((terms, volume_grad))
    coarse_kg, shared = call(collect, [((8, 3456), F32), ((group, 88, 128), BF16)], terms, far=(0,))
    shared = exchange(shared, "grp").reshape(1408, 128)
    fine_kg, down_kg = call(unpack, [((64, 1728), F32), ((512, 128), F32)], shared, far=(0, 1))
    coarse_out = jnp.swapaxes(out_rows, 1, 2)[:, None]
    return (coarse_out, volume_grad[None], fine_kg.T, down_kg, coarse_kg.T)


def solution(mesh):
    in_specs = (P("grp", "gz", None, None), P(None, "gz", None, "grp"), P(), P(), P(None, "grp"))
    out_specs = (P(None, "gz", None, "grp"), P("grp", "gz", None, None), P(), P(), P(None, "grp"))
    return jax.shard_map(
        per_device, mesh=mesh, in_specs=in_specs, out_specs=out_specs, check_vma=False
    )
```

```python
import jax
import jax.numpy as jnp
from jax import lax
from jax.experimental import pallas as pl
from jax.experimental.pallas import tpu as pltpu
from jax.sharding import PartitionSpec as P


F32 = jnp.float32
BF16 = jnp.bfloat16
NN = (((1,), (0,)), ((), ()))
NT = (((1,), (1,)), ((), ()))
TN = (((0,), (0,)), ((), ()))


def mm(left, right, dims):
    return lax.dot_general(left, right, dims, preferred_element_type=F32)


def shift_rows(value, by, period):
    total = value.shape[0]
    place = lax.broadcasted_iota(jnp.int32, value.shape, 0) % period
    inside = place != (0 if by == 1 else period - 1)
    return jnp.where(inside, pltpu.roll(value, by % total, 0), 0.0)


def low_half(rows):
    return lax.broadcasted_iota(jnp.int32, (rows, 128), 1) < 64


def slope_and_silu(pre):
    sig = jax.nn.sigmoid(pre)
    return sig * (1.0 + pre * (1.0 - sig)), pre * sig


def fill_windows(windows, plane, blocks):
    low = low_half(16)
    none = jnp.zeros((16, 128), BF16)
    for j in range(8):
        after = blocks[j + 1] if j < 7 else none
        before = blocks[j - 1] if j > 0 else none
        rows = pl.ds(j * 16, 16)
        windows[plane, rows, 0:128] = blocks[j]
        windows[plane, rows, 128:256] = jnp.where(low, after, before)


def window_conv(windows, weights, dims):
    parts = []
    for dx in range(3):
        total = None
        for dz in range(3):
            rows = windows[dz : dz + 2].reshape(256, 256)
            term = mm(rows, weights[dz * 3 + dx], dims)
            total = term if total is None else total + term
        parts.append(total)
    return parts[1] + shift_rows(parts[0], 1, 16) + shift_rows(parts[2], -1, 16)


def place_weights(kernel, ahead, behind):
    low = low_half(64)
    tiles = [kernel[:, m * 128 : (m + 1) * 128].astype(F32) for m in range(13)]
    last = kernel[:, 1664:1728].astype(F32)
    tiles.append(jnp.concatenate([last, jnp.zeros((64, 64), F32)], axis=1))
    for k in range(9):
        first, second = tiles[3 * k // 2], tiles[3 * k // 2 + 1]
        swapped = pltpu.roll(jnp.where(low, second, first), 64, 1)
        if k % 2 == 0:
            zero_one, two_none = first, jnp.where(low, second, 0.0)
            one_two, none_zero = swapped, pltpu.roll(jnp.where(low, first, 0.0), 64, 1)
        else:
            one_two, none_zero = second, jnp.where(low, 0.0, first)
            zero_one, two_none = swapped, pltpu.roll(jnp.where(low, 0.0, second), 64, 1)
        blocks = [part.astype(BF16) for part in (one_two, zero_one, none_zero, two_none)]
        ahead[k, 0:64, 0:128] = blocks[0]
        ahead[k, 64:128, 0:128] = blocks[1]
        ahead[k, 0:64, 128:256] = blocks[2]
        ahead[k, 64:128, 128:256] = blocks[3]
        for slot in range(4):
            behind[8 - k, slot * 64 : (slot + 1) * 64] = blocks[slot]


def sort_sides(core, near, far, sides):
    @pl.when(core[0] == 0)
    def _():
        sides[0] = far[...]
        sides[1] = near[...]

    @pl.when(core[0] == 1)
    def _():
        sides[0] = near[...]
        sides[1] = far[...]


def fine_forward(
    core, vol, near, far, weights, down, coarse, slope, windows, pooled, act, sides
):
    sort_sides(core, near, far, sides)

    def lanes(side, j):
        return sides[side, :, j * 128 : (j + 1) * 128]

    fill_windows(windows, 0, [lanes(0, j) for j in range(8)])
    fill_windows(windows, 1, [vol[0, :, j * 128 : (j + 1) * 128] for j in range(8)])
    fill_windows(windows, 2, [vol[1, :, j * 128 : (j + 1) * 128] for j in range(8)])
    fill_windows(windows, 3, [lanes(1, j) for j in range(8)])
    pre = window_conv(windows, weights, NT)
    slopes, silu = slope_and_silu(pre)
    slope[...] = slopes
    act[...] = silu
    for z in range(2):
        for bx in range(2):
            part = act[pl.ds(z * 128 + bx, 64, stride=2), :]
            at = (z * 2 + bx) * 128
            pooled[:, at : at + 128] = part.astype(BF16)
    coarse[...] = mm(pooled[...], down[...], NN).astype(BF16)


def y_taps(plane):
    value = plane[...].astype(F32)
    edge = jnp.zeros((8, 128), F32)
    earlier = jnp.concatenate([edge, value[:-8]], axis=0)
    later = jnp.concatenate([value[8:], edge], axis=0)
    return jnp.concatenate([earlier, value, later], axis=1).astype(BF16)


HALF = 1792


def spread_half(core, kernel, cotangent, out):
    for at in range(16):
        tail = jnp.concatenate([cotangent[at].astype(F32), jnp.zeros((8, 64), F32)], axis=1)
        out[at, :, HALF : HALF + 128] = tail.astype(BF16)

    @pl.when(core[0] == 0)
    def _():
        for at in range(16):
            out[at, :, 0:HALF] = kernel[:, 0:HALF]

    @pl.when(core[0] == 1)
    def _():
        for at in range(16):
            out[at, :, 0:HALF] = kernel[:, 3456 - HALF : 3456]


def insert_plane(mine, coarse_in, out):
    out[:, 0:HALF] = mine[:, 0:HALF]
    cotangent = mine[:, HALF : HALF + 128].astype(F32)[:, 0:64]
    plane = coarse_in[...].astype(F32).T
    out[:, HALF : HALF + 128] = jnp.concatenate([cotangent, plane], axis=1).astype(BF16)


def coarse_forward(
    core, own, far, mine, other, grad, out, packed, scratch, sides, near
):
    near[...] = other[:, HALF : HALF + 128].astype(F32).T[64:128].astype(BF16)
    sort_sides(core, near, far, sides)
    before, after = sides.at[0], sides.at[1]
    rest = 3456 - HALF

    @pl.when(core[0] == 0)
    def _():
        packed[:, 0:HALF] = mine[:, 0:HALF]
        packed[:, HALF:3456] = other[:, HALF - rest : HALF]

    @pl.when(core[0] == 1)
    def _():
        packed[:, 0:rest] = other[:, 0:rest]
        packed[:, rest:3456] = mine[:, 0:HALF]

    planes = [y_taps(before), y_taps(own), y_taps(after)]
    parts = []
    for dx in range(3):
        total = None
        for dz in range(3):
            at = (dz * 3 + dx) * 384
            term = mm(planes[dz], packed[:, at : at + 384], NT)
            total = term if total is None else total + term
        parts.append(total)
    pre = parts[1] + shift_rows(parts[0], 1, 8) + shift_rows(parts[2], -1, 8)
    slopes, silu = slope_and_silu(pre)
    scratch[0:64] = silu
    by_x = [scratch[pl.ds(x, 8, stride=8), :] for x in range(8)]
    scratch[...] = mine[:, HALF : HALF + 128].astype(F32).T
    cotangent = jnp.concatenate([scratch[pl.ds(y, 8, stride=8), :] for y in range(8)], axis=0)
    slopes = (cotangent * slopes).astype(BF16)
    grad[...] = slopes
    out[...] = jnp.concatenate(by_x + [slopes.astype(F32)], axis=0).T.astype(BF16)


def coarse_kernel_terms(parts, features, terms, grads, taps):
    low = low_half(8)
    place = lax.broadcasted_iota(jnp.int32, (8, 128), 1) % 8
    for volume in range(16):
        taps[volume * 64 : (volume + 1) * 64] = y_taps(parts[volume, 0:64])
        features[volume] = parts[volume, 64:72, 0:64]
    for pair in range(8):
        first = parts[pair * 2, 64:80].astype(F32)
        second = parts[pair * 2 + 1, 64:80].astype(F32)
        own = jnp.where(low, pltpu.roll(first[0:8], 64, 1), second[0:8])
        before = jnp.where(low, first[8:16], pltpu.roll(second[8:16], 64, 1))
        after = jnp.where(low, pltpu.roll(first[8:16], 64, 1), second[8:16])
        for dz, value in enumerate((after, own, before)):
            earlier = jnp.where(place != 7, pltpu.roll(value, 127, 1), 0.0)
            later = jnp.where(place != 0, pltpu.roll(value, 1, 1), 0.0)
            for dx, moved in enumerate((earlier, value, later)):
                at = (dz * 3 + dx) * 8
                grads[at : at + 8, pair * 128 : (pair + 1) * 128] = moved
    total = mm(grads[...].astype(BF16), taps[...], NN)
    shared = []
    for at in range(80, 160, 16):
        both = jnp.sum(parts[:, at : at + 16, :].astype(F32), axis=0)
        shared += [both[0:8], both[8:16]]
    shared.append(jnp.sum(parts[:, 160:168, :].astype(F32), axis=0))
    none = jnp.zeros((8, 128), F32)
    for device in range(32):
        k, dy = divmod(device, 3)
        own = total[k * 8 : k * 8 + 8, dy * 128 : (dy + 1) * 128] if device < 27 else none
        other = shared[device] if device < 11 else none
        terms[device] = jnp.concatenate([own, other], axis=0).astype(BF16)


def backward(
    core, own, near, far, packed, pooled, slope, windows, down, coarse_in, features,
    out, fine_grad, act, shared, sides,
):
    sort_sides(core, near, far, sides)
    before, after = sides.at[0], sides.at[1]
    planes = [after[...], own[...], before[...]]
    edge = jnp.zeros((8, 128), F32)
    parts = []
    for dx in range(3):
        total = None
        for dz in range(3):
            at = (dz * 3 + dx) * 384
            term = mm(planes[dz], packed[:, at : at + 384], NN)
            total = term if total is None else total + term
        earlier = jnp.concatenate([total[8:, 0:128], edge], axis=0)
        later = jnp.concatenate([edge, total[:-8, 256:384]], axis=0)
        parts.append(earlier + total[:, 128:256] + later)
    in_grad = parts[1] + shift_rows(parts[0], -1, 8) + shift_rows(parts[2], 1, 8)
    in_grad = in_grad.astype(BF16)
    act_grad = mm(in_grad, down[...], NT)
    for z in range(2):
        for bx in range(2):
            at = (z * 2 + bx) * 128
            act[pl.ds(z * 128 + bx, 64, stride=2), :] = act_grad[:, at : at + 128]
    grad = (act[...] * slope[...]).astype(BF16)
    fine_grad[0] = grad[0:128]
    fine_grad[1] = grad[128:256]
    value = grad.astype(F32)
    moved = [shift_rows(value, -1, 16), value, shift_rows(value, 1, 16)]
    moved = [part.astype(BF16) for part in moved]
    low = low_half(64)
    held = None
    for dz in range(3):
        rows = windows[dz : dz + 2].reshape(256, 256)
        for dx in range(3):
            block = mm(moved[dx], rows, TN)
            u0, u1 = block[0:64, 0:128], block[0:64, 128:256]
            v0, v1 = block[64:128, 0:128], block[64:128, 128:256]
            for dy, (left, right) in enumerate(((u1, v0), (v0, u0), (u0, v1))):
                tap = (dz * 3 + dx) * 3 + dy
                if tap % 2 == 0:
                    held = pltpu.roll(left, 64, 1) + right
                else:
                    high = left + pltpu.roll(right, 64, 1)
                    at = (tap // 2) * 64
                    shared[at : at + 64] = jnp.where(low, held, high)
    shared[832:896] = jnp.where(low, held, 0.0)
    shared[896:1408] = mm(pooled[...], in_grad, TN)
    sides = jnp.concatenate([before[...].astype(F32), after[...].astype(F32)], axis=0).T
    for at in range(16):
        rows = slice(at * 8, at * 8 + 8)
        out[at, 0:64] = coarse_in[...]
        mixed = jnp.concatenate([features[rows].astype(F32), sides[rows]], axis=0)
        out[at, 64:80] = mixed.astype(BF16)
        out[at, 80:168] = shared[at * 88 : at * 88 + 88].astype(BF16)


def fine_backward(core, grad, near, far, weights, out, windows, sides):
    sort_sides(core, near, far, sides)

    def blocks(plane):
        return [plane[j * 16 : (j + 1) * 16] for j in range(8)]

    fill_windows(windows, 0, blocks(sides[0]))
    fill_windows(windows, 1, blocks(grad[0]))
    fill_windows(windows, 2, blocks(grad[1]))
    fill_windows(windows, 3, blocks(sides[1]))
    total = window_conv(windows, weights, NN).astype(BF16)
    for z in range(2):
        for j in range(8):
            at = z * 128 + j * 16
            out[z, :, j * 128 : (j + 1) * 128] = total[at : at + 16]


def sum_slabs(terms, out):
    total = jnp.sum(terms[...].astype(F32), axis=0).astype(BF16)
    for device in range(32):
        out[device] = total


def collect(terms, coarse, out):
    rows = []
    for device in range(27):
        both = terms[device].astype(F32)
        coarse[:, device * 128 : (device + 1) * 128] = both[0:8]
        rows.append(both[8:16])
    total = jnp.concatenate(rows[0:11], axis=0).astype(BF16)
    for device in range(16):
        out[device] = total


def unpack(shared, fine, down):
    for tile in range(13):
        rows = shared[tile * 64 : (tile + 1) * 64]
        fine[:, tile * 128 : (tile + 1) * 128] = rows.astype(F32)
    fine[:, 1664:1728] = shared[832:896].astype(F32)[:, 0:64]
    down[...] = shared[896:1408].astype(F32)


def call(body, outs, *operands, scratch=(), far=(), core=None, moved=True):
    place = [jax.ShapeDtypeStruct if at in far else pltpu.VMEM for at in range(len(outs))]
    first = [] if core is None else [core]
    if moved:
        operands = [pltpu.with_memory_space_constraint(part, pltpu.VMEM) for part in operands]
    specs = [pl.BlockSpec(memory_space=pltpu.SMEM) for _ in first]
    return pl.pallas_call(
        body,
        out_shape=[put(*out) for put, out in zip(place, outs)],
        in_specs=specs + [pl.BlockSpec(memory_space=pltpu.VMEM) for _ in operands],
        scratch_shapes=[pltpu.VMEM(shape, kind) for shape, kind in scratch],
        cost_estimate=pl.CostEstimate(flops=WORK, transcendentals=0, bytes_accessed=1 << 20),
        interpret=INTERPRET,
    )(*first, *operands)


INTERPRET = False
WORK = 250_000_000


def core_swap(array):
    return lax.ppermute(array, "gz", [(i, i ^ 1) for i in range(lax.axis_size("gz"))])


def other_swap(array):
    up = [(i, i + 1) for i in range(1, lax.axis_size("gz") - 1, 2)]
    return lax.ppermute(array, "gz", up + [(j, i) for i, j in up])


def pair_swaps(to_core, to_other):
    return core_swap(to_core), other_swap(to_other)


def exchange(blocks, axis):
    return lax.all_to_all(blocks, axis, 0, 0, tiled=True)


def per_device(volumes, cotangent, fine_kernel, down_kernel, coarse_kernel):
    group = lax.axis_size("grp")
    slabs = lax.axis_size("gz")
    vol = volumes[0]
    core = (lax.axis_index("gz") & 1).astype(jnp.int32).reshape(1)
    (halves,) = call(
        spread_half,
        [((group, 8, HALF + 128), BF16)],
        coarse_kernel.T, jnp.swapaxes(cotangent[:, 0], 1, 2),
        core=core,
        moved=False,
    )
    index = core[0]
    near, far = pair_swaps(
        lax.dynamic_index_in_dim(vol, 1 - index, 0, keepdims=False),
        lax.dynamic_index_in_dim(vol, index, 0, keepdims=False),
    )
    mine = exchange(halves, "grp").reshape(128, HALF + 128)
    ahead, behind = call(
        place_weights, [((9, 128, 256), BF16), ((9, 256, 128), BF16)], fine_kernel.T, far=(1,)
    )

    coarse_in, slope, windows, pooled = call(
        fine_forward,
        [((64, 128), BF16), ((256, 128), F32), ((4, 128, 256), BF16), ((64, 512), BF16)],
        vol, near, far, ahead, down_kernel,
        scratch=[((256, 128), F32), ((2, 16, 1024), BF16)],
        core=core,
        far=(1, 2),
    )
    in_far = other_swap(coarse_in)
    (mine,) = call(insert_plane, [((128, HALF + 128), BF16)], mine, coarse_in)
    other = core_swap(mine)
    coarse_grad, features, packed = call(
        coarse_forward,
        [((64, 128), BF16), ((128, 128), BF16), ((128, 3456), BF16)],
        coarse_in, in_far, mine, other,
        scratch=[((128, 128), F32), ((2, 64, 128), BF16), ((64, 128), BF16)],
        core=core,
    )
    grad_near, grad_far = pair_swaps(coarse_grad, coarse_grad)
    parts, fine_grad = call(
        backward,
        [((group, 168, 128), BF16), ((2, 128, 128), BF16)],
        coarse_grad, grad_near, grad_far, packed, pooled, slope, windows, down_kernel,
        coarse_in, features,
        scratch=[((256, 128), F32), ((1408, 128), F32), ((2, 64, 128), BF16)],
        core=core,
    )
    parts = exchange(parts, "grp")
    fine_near, fine_far = pair_swaps(
        lax.dynamic_index_in_dim(fine_grad, 1 - index, 0, keepdims=False),
        lax.dynamic_index_in_dim(fine_grad, index, 0, keepdims=False),
    )
    (volume_grad,) = call(
        fine_backward,
        [((2, 16, 1024), BF16)],
        fine_grad, fine_near, fine_far, behind,
        scratch=[((4, 128, 256), BF16), ((2, 128, 128), BF16)],
        core=core,
        far=(0,),
    )
    parts, volume_grad = lax.optimization_barrier((parts, volume_grad))
    out_rows, terms = call(
        coarse_kernel_terms,
        [((group, 8, 64), BF16), ((slabs, 16, 128), BF16)],
        parts,
        scratch=[((72, 1024), F32), ((1024, 384), BF16)],
        far=(0,),
    )
    terms = exchange(terms, "gz")
    (terms,) = call(sum_slabs, [((slabs, 16, 128), BF16)], terms)
    terms = exchange(terms, "gz")
    coarse_kg, shared = call(collect, [((8, 3456), F32), ((group, 88, 128), BF16)], terms, far=(0,))
    shared = exchange(shared, "grp").reshape(1408, 128)
    fine_kg, down_kg = call(unpack, [((64, 1728), F32), ((512, 128), F32)], shared, far=(0, 1))
    coarse_out = jnp.swapaxes(out_rows, 1, 2)[:, None]
    return (coarse_out, volume_grad[None], fine_kg.T, down_kg, coarse_kg.T)


def solution(mesh):
    in_specs = (P("grp", "gz", None, None), P(None, "gz", None, "grp"), P(), P(), P(None, "grp"))
    out_specs = (P(None, "gz", None, "grp"), P("grp", "gz", None, None), P(), P(), P(None, "grp"))
    return jax.shard_map(
        per_device, mesh=mesh, in_specs=in_specs, out_specs=out_specs, check_vma=False
    )
```
